128 devices in a mesh: blk: 16 (over y, x_hi, core), ulysses: 8 (over x_lo, z).
Axes of the slice: x: 4 (x_hi: 2, x_lo: 2; x = x_hi * 2 + x_lo), y: 4, z: 4, core: 2. Of those that a mesh axis runs over, the one named last changes fastest.
Arguments:
- tokens: bfloat16 [8192, 3072], P(('blk', 'ulysses')), may hold values from -6 to 6
- mod_shift: float32 [3072], replicated, may hold values from -3 to 3
- mod_scale: float32 [3072], replicated, may hold values from -3 to 3
- mod_gate: float32 [3072], replicated, may hold values from 0.5 to 1.5
- qkv_weight: bfloat16 [3, 3072, 3072], P(None, None, 'ulysses'), may hold values from -0.109375 to 0.109375
- query_gain: float32 [128], replicated, may hold values from 1 to 16
- key_gain: float32 [128], replicated, may hold values from 1 to 16
- out_weight: bfloat16 [3072, 3072], P(None, 'ulysses'), may hold values from -0.109375 to 0.109375
Outputs:
- mixed: bfloat16 [8192, 3072], P(('blk', 'ulysses'))
The draws below stay inside these ranges and needn't reach their ends.
All inputs are finite; a program needn't handle non-finite values.
Results may differ from the reference program's by a relative error of at most 0.013.
The reference program's roundings to bfloat16 on the way (of `modulated`, `queries`, `keys`, `values`, `powers` and `attended`) count: a program that leaves them out, or rounds other values in their place, can miss the bound.
Values may be sent and summed in bfloat16 or wider, within the bound.
A program may use at most 128 MiB of HBM per device.

```python
import math
import jax
import jax.numpy as jnp
from jax import lax

D = 3072
HEADS = 24
HEAD_DIM = 128
SEQ = 8192


def gain_vector(key, salt):
    base = jnp.exp(jax.random.uniform(jax.random.fold_in(key, salt), (HEAD_DIM,), jnp.float32, 0.0, 1.1))
    return base


def draw_query_gain(key, part):
    return gain_vector(key, 1)


def draw_key_gain(key, part):
    return gain_vector(key, 2)


def block_levels(stream_key, shape, shards, smallest, high):
    factor_of = 1.0
    for dim, blocks in shards:
        heights = jax.random.uniform(jax.random.fold_in(jax.random.fold_in(stream_key, 6), dim), (blocks,), jnp.float32, smallest / len(shards), high / len(shards))
        factor_of = factor_of * jnp.repeat(jnp.exp(heights), shape[dim] // blocks).reshape((-1,) + (1,) * (len(shape) - 1 - dim))
    return factor_of


def bell_draw(stream_key, shape, width, bound, cuts=(), held_as=jnp.bfloat16):
    loudness = block_levels(stream_key, shape, cuts, -0.22, 0.18) if cuts else 1.0
    values = jax.random.normal(stream_key, shape, jnp.float32) * width * loudness
    return jnp.minimum(jnp.maximum(values, -bound), bound).astype(held_as)


def setup_inputs(seed: int = 0) -> dict:
    streams_of = jax.random.split(jax.random.key(seed), 9)
    return {
        "tokens": bell_draw(streams_of[0], (SEQ, D), 1.0, 6.0, ((0, 128),)),
        "mod_shift": bell_draw(streams_of[1], (D,), 0.5, 3.0, (), jnp.float32),
        "mod_scale": bell_draw(streams_of[2], (D,), 0.5, 3.0, (), jnp.float32),
        "mod_gate": jnp.clip(jax.random.uniform(streams_of[3], (D,), jnp.float32, 0.5, 1.5), 0.5, 1.5),
        "qkv_weight": bell_draw(streams_of[4], (3, D, HEADS * HEAD_DIM), D ** -0.5, 0.109375, ((2, 8),)),
        "query_gain": draw_query_gain(jax.random.fold_in(streams_of[8], 71), 0),
        "key_gain": draw_key_gain(jax.random.fold_in(streams_of[8], 71), 0),
        "out_weight": bell_draw(streams_of[7], (HEADS * HEAD_DIM, D), (HEADS * HEAD_DIM) ** -0.5, 0.109375, ((1, 8),)),
    }


def head_norm(projected, gain, factor):
    split = projected.reshape(projected.shape[0], -1, gain.shape[0])
    meansq = lax.optimization_barrier(jnp.mean(split * split, axis=-1, keepdims=True))
    return (split * lax.rsqrt(meansq + 1e-06) * gain * factor).reshape(projected.shape)

def reference(tokens, mod_shift, mod_scale, mod_gate, qkv_weight, query_gain, key_gain, out_weight):
    wide = tokens.astype(jnp.float32)
    center = lax.optimization_barrier(jnp.mean(wide, axis=-1, keepdims=True))
    spread = lax.optimization_barrier(jnp.mean((wide - center) ** 2, axis=-1, keepdims=True))
    normed = (wide - center) / jnp.sqrt(spread + 1e-06)
    modulated = (normed * (1.0 + mod_scale) + mod_shift).astype(jnp.bfloat16)
    query_sums = jnp.dot(modulated, qkv_weight[0], preferred_element_type=jnp.float32)
    key_sums = jnp.dot(modulated, qkv_weight[1], preferred_element_type=jnp.float32)
    value_sums = jnp.dot(modulated, qkv_weight[2], preferred_element_type=jnp.float32)
    queries = head_norm(query_sums, query_gain, 1.0 / math.sqrt(HEAD_DIM)).astype(jnp.bfloat16)
    keys = head_norm(key_sums, key_gain, 1.0).astype(jnp.bfloat16)
    values = value_sums.astype(jnp.bfloat16)
    length = tokens.shape[0]
    block = math.gcd(length, 1024)

    def heads_first(matrix):
        return matrix.reshape(length, HEADS, HEAD_DIM).transpose(1, 0, 2)

    def one_head(operands):
        query_head, key_head, value_head = operands

        def one_block(query_block):
            scores = jnp.dot(query_block, key_head.T, preferred_element_type=jnp.float32)
            highest = lax.optimization_barrier(jnp.max(scores, axis=-1, keepdims=True))
            powers = jnp.exp(scores - highest)
            numerator = jnp.dot(powers.astype(jnp.bfloat16), value_head, preferred_element_type=jnp.float32)
            return numerator / lax.optimization_barrier(jnp.sum(powers, axis=-1, keepdims=True))
        result = lax.map(one_block, query_head.reshape(length // block, block, HEAD_DIM))
        return result.reshape(length, HEAD_DIM)
    attended = lax.map(one_head, (heads_first(queries), heads_first(keys), heads_first(values)))
    attended = attended.transpose(1, 0, 2).reshape(length, HEADS * HEAD_DIM).astype(jnp.bfloat16)
    branch = jnp.dot(attended, out_weight, preferred_element_type=jnp.float32)
    return (wide + mod_gate * branch).astype(jnp.bfloat16)
```

```python
import math

import jax
import jax.numpy as jnp
from jax import lax
from jax.experimental import pallas as pl
from jax.experimental.pallas import tpu as pltpu
from jax.sharding import PartitionSpec as P

MESH = pl.DeviceIdType.MESH
F32 = jnp.float32
BF16 = jnp.bfloat16
NT = (((1,), (1,)), ((), ()))


def kernel(
    tokens_ref, shift_ref, scale_ref, gate_ref, qgain_ref, kgain_ref, w_hbm, wo_hbm,
    out_ref,
    w, wo, mod, q, kv, att, outb, drec, m_s, l_s, acc, oacc,
    w_sem, a_ssem, a_rsem, b_ssem, b_rsem, c_ssem, c_rsem, d_ssem, d_rsem,
):
    blk = lax.axis_index("blk")
    u = lax.axis_index("ulysses")
    y, xh, core = blk // 4, (blk // 2) % 2, blk % 2
    xl, z = u // 4, u % 4
    x = xh * 2 + xl

    def device(x_, y_, z_, c_):
        return (y_ * 4 + (x_ // 2) * 2 + c_, (x_ % 2) * 4 + z_)

    zp, zm, z2 = (z + 1) % 4, (z + 3) % 4, (z + 2) % 4
    xp, xm, x2 = (x + 1) % 4, (x + 3) % 4, (x + 2) % 4
    yp, ym = (y + 1) % 4, (y + 3) % 4
    dev_zp, dev_zm = device(x, y, zp, core), device(x, y, zm, core)
    dev_xp, dev_xm = device(xp, y, z, core), device(xm, y, z, core)
    dev_x2 = device(x2, y, z, core)
    dev_yp, dev_ym = device(x, yp, z, core), device(x, ym, z, core)
    dev_core = device(x, y, z, 1 - core)

    w_copies = [
        pltpu.make_async_copy(w_hbm.at[j], w.at[:, pl.ds(j * 384, 384)], w_sem.at[j]) for j in range(3)
    ]
    w_copies.append(pltpu.make_async_copy(wo_hbm, wo, w_sem.at[3]))
    for c_ in w_copies:
        c_.start()

    wide = tokens_ref[...].astype(F32)
    center = jnp.mean(wide, axis=-1, keepdims=True)
    spread = jnp.mean((wide - center) ** 2, axis=-1, keepdims=True)
    normed = (wide - center) / jnp.sqrt(spread + 1e-06)
    modulated = (normed * (1.0 + scale_ref[...]) + shift_ref[...]).astype(BF16)
    mod[z] = modulated[:32]
    mod[12 + z] = modulated[32:]

    barrier = pltpu.get_barrier_semaphore()
    partners = [dev_yp, dev_ym, dev_x2, dev_core]
    for d in range(4):
        zd = (z + d) % 4
        if d:
            partners.append(device(x, y, zd, core))
        partners.append(device(xp, y, zd, core))
        partners.append(device(xm, y, zd, core))
    for p in partners:
        pl.semaphore_signal(barrier, inc=1, device_id=p, device_id_type=MESH)
    pl.semaphore_wait(barrier, len(partners))

    sends = []

    def make(src, dst, ssem, rsem, dev):
        return pltpu.make_async_remote_copy(
            src_ref=src, dst_ref=dst, send_sem=ssem, recv_sem=rsem, device_id=dev, device_id_type=MESH
        )

    def send(src, dst, ssem, rsem, dev):
        c_ = make(src, dst, ssem, rsem, dev)
        c_.start()
        sends.append(c_)

    class Gather:
        def __init__(self, own_a, own_b, from_minus, from_plus, ssem, rsem):
            self.a, self.b, self.fm, self.fp = own_a, own_b, from_minus, from_plus
            self.ssem, self.rsem = ssem, rsem

        def send(self, t, src, dst, dev):
            send(src, dst, self.ssem.at[t], self.rsem.at[t], dev)

        def recv(self, t, dst):
            make(dst, dst, self.ssem.at[t], self.rsem.at[t], dev_zp).wait_recv()

        def start(self):
            self.send(0, self.a(z), self.a(z), dev_zp)
            self.send(2, self.b(z), self.b(z), dev_zm)
            self.send(4, self.a(z), self.fm(z), dev_xp)
            self.send(5, self.b(z), self.fp(z), dev_xm)
            self.send(1, self.b(z), self.b(z), dev_zp)
            self.send(3, self.a(z), self.a(z), dev_zm)

        def wave1(self):
            self.recv(0, self.a(zm))
            self.send(7, self.a(zm), self.fm(zm), dev_xp)
            self.send(6, self.a(zm), self.a(zm), dev_zp)
            self.recv(2, self.b(zp))
            self.send(9, self.b(zp), self.fp(zp), dev_xm)
            self.send(8, self.b(zp), self.b(zp), dev_zm)

        def x_own(self):
            self.recv(4, self.fm(z))
            self.recv(5, self.fp(z))

        def wave2(self):
            self.recv(3, self.a(zp))
            self.send(10, self.a(zp), self.fm(zp), dev_xp)
            self.recv(1, self.b(zm))
            self.send(11, self.b(zm), self.fp(zm), dev_xm)

        def wave3(self):
            self.recv(6, self.a(z2))
            self.send(12, self.a(z2), self.fm(z2), dev_xp)
            self.recv(8, self.b(z2))
            self.send(13, self.b(z2), self.fp(z2), dev_xm)

        def x_near(self):
            self.recv(7, self.fm(zm))
            self.recv(9, self.fp(zp))
            self.recv(10, self.fm(zp))
            self.recv(11, self.fp(zm))

        def x_far(self):
            self.recv(12, self.fm(z2))
            self.recv(13, self.fp(z2))

    factor = 1.0 / math.sqrt(128)

    def head_norm(value, gain):
        meansq = jnp.mean(value * value, axis=-1, keepdims=True)
        return value * lax.rsqrt(meansq + 1e-06) * gain

    def project(g, pieces):
        rows = jnp.concatenate([mod[p] for p in pieces], axis=0)
        sums = jnp.dot(rows, w[...], preferred_element_type=F32)
        for h in range(3):
            qh = (head_norm(sums[:, h * 128:h * 128 + 128], qgain_ref[...]) * factor).astype(BF16)
            for i, p in enumerate(pieces):
                q[h, p] = qh[i * 32:i * 32 + 32]
            kh = head_norm(sums[:, 384 + h * 128:384 + h * 128 + 128], kgain_ref[...])
            kv[h, 0, g, 0] = kh.astype(BF16)
            vh = sums[:, 768 + h * 128:768 + h * 128 + 128]
            kv[h, 0, g, 1] = vh.T.astype(BF16)

    ga = Gather(
        lambda i: mod.at[i], lambda i: mod.at[12 + i], lambda i: mod.at[8 + i], lambda i: mod.at[4 + i],
        a_ssem, a_rsem,
    )
    ga.start()
    for c_ in w_copies:
        c_.wait()
    ga.wave1()
    ga.x_own()
    project(0, [z, 12 + z, 8 + z, 4 + z])
    ga.wave2()
    project(1, [zm, 12 + zm, zp, 12 + zp])
    ga.wave3()
    ga.x_near()
    project(2, [8 + zm, 4 + zm, 8 + zp, 4 + zp])
    ga.x_far()
    project(3, [z2, 12 + z2, 8 + z2, 4 + z2])

    def b_send(h, t, src, dst, dev):
        send(src, dst, b_ssem.at[h, t], b_rsem.at[h, t], dev)

    def b_recv(h, t, dst):
        make(dst, dst, b_ssem.at[h, t], b_rsem.at[h, t], dev_yp).wait_recv()

    lo, hi = pl.ds(0, 2), pl.ds(2, 2)
    for h in range(3):
        own = kv.at[h, 0]
        b_send(h, 2, own, kv.at[h, 4], dev_x2)
        b_send(h, 0, own, kv.at[h, 3], dev_yp)
        b_send(h, 1, own, kv.at[h, 1], dev_ym)
        b_send(h, 3, own, kv.at[h, 8], dev_core)

    def b_event(h, e):
        at = lambda s: kv.at[h, s]
        if e == 0:
            b_recv(h, 0, at(3))
            b_send(h, 4, kv.at[h, 3, lo], kv.at[h, 2, lo], dev_yp)
            b_send(h, 5, at(3), at(11), dev_core)
            b_recv(h, 1, at(1))
            b_send(h, 6, kv.at[h, 1, hi], kv.at[h, 2, hi], dev_ym)
            b_send(h, 7, at(1), at(9), dev_core)
        if e == 1:
            b_recv(h, 2, at(4))
            b_send(h, 8, at(4), at(7), dev_yp)
            b_send(h, 9, at(4), at(5), dev_ym)
            b_send(h, 10, at(4), at(12), dev_core)
        if e == 2:
            b_recv(h, 8, at(7))
            b_send(h, 11, kv.at[h, 7, lo], kv.at[h, 6, lo], dev_yp)
            b_send(h, 12, at(7), at(15), dev_core)
            b_recv(h, 9, at(5))
            b_send(h, 13, kv.at[h, 5, hi], kv.at[h, 6, hi], dev_ym)
            b_send(h, 14, at(5), at(13), dev_core)
        if e == 3:
            b_recv(h, 4, kv.at[h, 2, lo])
            b_recv(h, 6, kv.at[h, 2, hi])
            b_send(h, 15, at(2), at(10), dev_core)
        if e == 4:
            b_recv(h, 11, kv.at[h, 6, lo])
            b_recv(h, 13, kv.at[h, 6, hi])
            b_send(h, 16, at(6), at(14), dev_core)
        if e == 5:
            for t, s in ((3, 8), (5, 11), (7, 9), (10, 12), (12, 15), (14, 13), (15, 10), (16, 14)):
                b_recv(h, t, at(s))

    def attend(h):
        m_s[...] = jnp.full_like(m_s, -1e30)
        l_s[...] = jnp.zeros_like(l_s)
        acc[...] = jnp.zeros_like(acc)

        def body(s, carry):
            keys = jnp.concatenate([kv[h, s, g, 0] for g in range(4)], axis=0)
            vals = jnp.concatenate([kv[h, s, g, 1] for g in range(4)], axis=1)
            for half in range(2):
                cols = pl.ds(half * 256, 256)
                queries = q[h, pl.ds(half * 8, 8)].reshape(256, 128)
                scores = lax.dot_general(keys, queries, NT, preferred_element_type=F32)
                old = m_s[:, cols]
                new = jnp.maximum(old, jnp.max(scores, axis=0, keepdims=True))
                rescale = jnp.exp(old - new)
                powers = jnp.exp(scores - new)
                m_s[:, cols] = new
                l_s[:, cols] = l_s[:, cols] * rescale + jnp.sum(powers, axis=0, keepdims=True)
                acc[:, cols] = acc[:, cols] * rescale + jnp.dot(
                    vals, powers.astype(BF16), preferred_element_type=F32
                )
            return carry

        lax.fori_loop(0, 16, body, 0)
        result = (acc[...] / l_s[...]).T.astype(BF16)
        att[h, 0, z, 0] = result[:256]
        att[h, 0, z, 1] = result[256:]

    gathers = []
    for h in range(3):
        gc = Gather(
            lambda i, h=h: att.at[h, 0, i, 0], lambda i, h=h: att.at[h, 0, i, 1],
            lambda i, h=h: att.at[h, 1, i, 1], lambda i, h=h: att.at[h, 1, i, 0],
            c_ssem.at[h], c_rsem.at[h],
        )
        gathers.append(gc)

    for e in range(6):
        b_event(0, e)
    attend(0)
    gathers[0].start()
    for e in range(6):
        b_event(1, e)
    gathers[0].wave1()
    gathers[0].wave2()
    attend(1)
    gathers[1].start()
    for e in range(6):
        b_event(2, e)
    gathers[0].wave3()
    gathers[1].wave1()
    gathers[1].wave2()
    attend(2)
    gathers[2].start()
    gathers[1].wave3()

    def project_out(h, first):
        def body(i, carry):
            z0 = i
            rows = jnp.concatenate(
                [att[h, c_, z0].reshape(512, 128) for c_ in range(2)], axis=1
            )
            weights = jnp.concatenate([wo[(xl * 4 + z0) * 3 + h], wo[((1 - xl) * 4 + z0) * 3 + h]], axis=0)
            oacc[...] += jnp.dot(rows, weights, preferred_element_type=F32)
            return carry

        lax.fori_loop(0, 4, body, 0)

    oacc[...] = jnp.zeros_like(oacc)
    for h in range(3):
        if h == 2:
            gathers[2].wave1()
            gathers[2].wave2()
            gathers[2].wave3()
        gathers[h].x_own()
        gathers[h].x_near()
        gathers[h].x_far()
        project_out(h, h == 0)

    outb[...] = oacc[...].astype(BF16).reshape(16, 32, 384)
    for d in range(4):
        zd = (z + d) % 4
        if d == 0:
            drec[0, u] = outb[z]
            drec[1, u] = outb[12 + z]
        else:
            dev = device(x, y, zd, core)
            send(outb.at[zd], drec.at[0, u], d_ssem.at[0, d], d_rsem.at[0, d], dev)
            send(outb.at[12 + zd], drec.at[1, u], d_ssem.at[1, d], d_rsem.at[1, d], dev)
        send(outb.at[8 + zd], drec.at[0, u], d_ssem.at[2, d], d_rsem.at[2, d], device(xm, y, zd, core))
        send(outb.at[4 + zd], drec.at[1, u], d_ssem.at[3, d], d_rsem.at[3, d], device(xp, y, zd, core))
    for d in range(4):
        zs = (z + 4 - d) % 4
        for kind in range(4):
            if d == 0 and kind < 2:
                continue
            dst = drec.at[kind % 2, (xl if kind < 2 else 1 - xl) * 4 + zs]
            make(dst, dst, d_ssem.at[kind, d], d_rsem.at[kind, d], dev_zp).wait_recv()
    for v in range(8):
        cols = pl.ds(v * 384, 384)
        branch = jnp.concatenate([drec[0, v], drec[1, v]], axis=0).astype(F32)
        out_ref[:, cols] = (tokens_ref[:, cols].astype(F32) + gate_ref[:, cols] * branch).astype(BF16)

    for c_ in sends:
        c_.wait_send()


def local(tokens, mod_shift, mod_scale, mod_gate, qkv_weight, query_gain, key_gain, out_weight):
    vm = pl.BlockSpec(memory_space=pltpu.VMEM)
    anyspace = pl.BlockSpec(memory_space=pl.ANY)
    dma = pltpu.SemaphoreType.DMA
    return pl.pallas_call(
        kernel,
        out_shape=jax.ShapeDtypeStruct(tokens.shape, BF16),
        in_specs=[vm] * 6 + [anyspace] * 2,
        out_specs=vm,
        scratch_shapes=[
            pltpu.VMEM((3072, 1152), BF16),
            pltpu.VMEM((24, 128, 384), BF16),
            pltpu.VMEM((16, 32, 3072), BF16),
            pltpu.VMEM((3, 16, 32, 128), BF16),
            pltpu.VMEM((3, 16, 4, 2, 128, 128), BF16),
            pltpu.VMEM((3, 2, 4, 2, 256, 128), BF16),
            pltpu.VMEM((16, 32, 384), BF16),
            pltpu.VMEM((2, 8, 32, 384), BF16),
            pltpu.VMEM((1, 512), F32),
            pltpu.VMEM((1, 512), F32),
            pltpu.VMEM((128, 512), F32),
            pltpu.VMEM((512, 384), F32),
            dma((4,)),
            dma((14,)), dma((14,)),
            dma((3, 17)), dma((3, 17)),
            dma((3, 14)), dma((3, 14)),
            dma((4, 4)), dma((4, 4)),
        ],
        compiler_params=pltpu.CompilerParams(
            collective_id=0, has_side_effects=True, vmem_limit_bytes=60 * 1024 * 1024
        ),
        name="joint_attention",
    )(
        tokens, mod_shift.reshape(1, -1), mod_scale.reshape(1, -1), mod_gate.reshape(1, -1),
        query_gain.reshape(1, -1), key_gain.reshape(1, -1), qkv_weight, out_weight.reshape(24, 128, 384),
    )


def solution(mesh):
    in_specs = (
        P(("blk", "ulysses"), None),
        P(),
        P(),
        P(),
        P(None, None, "ulysses"),
        P(),
        P(),
        P(None, "ulysses"),
    )
    out_specs = P(("blk", "ulysses"), None)
    return jax.shard_map(local, mesh=mesh, in_specs=in_specs, out_specs=out_specs, check_vma=False)
```

```python
import math

import jax
import jax.numpy as jnp
from jax import lax
from jax.experimental import pallas as pl
from jax.experimental.pallas import tpu as pltpu
from jax.sharding import PartitionSpec as P

MESH = pl.DeviceIdType.MESH
F32 = jnp.float32
BF16 = jnp.bfloat16
NT = (((1,), (1,)), ((), ()))


def kernel(
    tokens_ref, shift_ref, scale_ref, gate_ref, qgain_ref, kgain_ref, w_hbm, wo_hbm,
    out_ref,
    w, wo, mod, q, kv, att, outb, drec, m_s, l_s, acc, s_s, osend, orecv, stsend, strecv, oacc,
    w_sem, a_ssem, a_rsem, o_ssem, o_rsem, f_ssem, f_rsem, q_ssem, q_rsem, e_ssem, e_rsem,
    c_ssem, c_rsem, d_ssem, d_rsem,
):
    blk = lax.axis_index("blk")
    u = lax.axis_index("ulysses")
    y, xh, core = blk // 4, (blk // 2) % 2, blk % 2
    xl, z = u // 4, u % 4
    x = xh * 2 + xl

    def device(x_, y_, z_, c_):
        return (y_ * 4 + (x_ // 2) * 2 + c_, (x_ % 2) * 4 + z_)

    zp, zm, z2 = (z + 1) % 4, (z + 3) % 4, (z + 2) % 4
    xp, xm, x2 = (x + 1) % 4, (x + 3) % 4, (x + 2) % 4
    yp, ym = (y + 1) % 4, (y + 3) % 4
    dev_zp, dev_zm = device(x, y, zp, core), device(x, y, zm, core)
    dev_xp, dev_xm = device(xp, y, z, core), device(xm, y, z, core)
    dev_x2 = device(x2, y, z, core)
    dev_yp, dev_ym = device(x, yp, z, core), device(x, ym, z, core)
    dev_core = device(x, y, z, 1 - core)

    w_copies = [
        pltpu.make_async_copy(w_hbm.at[j], w.at[:, pl.ds(j * 384, 384)], w_sem.at[j]) for j in range(3)
    ]
    w_copies.append(pltpu.make_async_copy(wo_hbm, wo, w_sem.at[3]))
    for c_ in w_copies:
        c_.start()

    wide = tokens_ref[...].astype(F32)
    center = jnp.mean(wide, axis=-1, keepdims=True)
    spread = jnp.mean((wide - center) ** 2, axis=-1, keepdims=True)
    normed = (wide - center) / jnp.sqrt(spread + 1e-06)
    modulated = (normed * (1.0 + scale_ref[...]) + shift_ref[...]).astype(BF16)
    mod[z] = modulated[:32]
    mod[12 + z] = modulated[32:]

    barrier = pltpu.get_barrier_semaphore()
    partners = [dev_yp, dev_ym, dev_x2, dev_core]
    for d in range(4):
        zd = (z + d) % 4
        if d:
            partners.append(device(x, y, zd, core))
        partners.append(device(xp, y, zd, core))
        partners.append(device(xm, y, zd, core))
    for p in partners:
        pl.semaphore_signal(barrier, inc=1, device_id=p, device_id_type=MESH)
    pl.semaphore_wait(barrier, len(partners))

    def make(src, dst, ssem, rsem, dev):
        return pltpu.make_async_remote_copy(
            src_ref=src, dst_ref=dst, send_sem=ssem, recv_sem=rsem, device_id=dev, device_id_type=MESH
        )

    def send(src, dst, ssem, rsem, dev):
        make(src, dst, ssem, rsem, dev).start()

    def sent(src, ssem, rsem):
        make(src, src, ssem, rsem, dev_zp).wait_send()

    class Gather:
        def __init__(self, own_a, own_b, from_minus, from_plus, ssem, rsem):
            self.a, self.b, self.fm, self.fp = own_a, own_b, from_minus, from_plus
            self.ssem, self.rsem = ssem, rsem

        def send(self, t, src, dst, dev):
            send(src, dst, self.ssem.at[t], self.rsem.at[t], dev)

        def recv(self, t, dst):
            make(dst, dst, self.ssem.at[t], self.rsem.at[t], dev_zp).wait_recv()

        def start(self):
            self.send(0, self.a(z), self.a(z), dev_zp)
            self.send(2, self.b(z), self.b(z), dev_zm)
            self.send(4, self.a(z), self.fm(z), dev_xp)
            self.send(5, self.b(z), self.fp(z), dev_xm)
            self.send(1, self.b(z), self.b(z), dev_zp)
            self.send(3, self.a(z), self.a(z), dev_zm)

        def wave1(self):
            self.recv(0, self.a(zm))
            self.send(7, self.a(zm), self.fm(zm), dev_xp)
            self.send(6, self.a(zm), self.a(zm), dev_zp)
            self.recv(2, self.b(zp))
            self.send(9, self.b(zp), self.fp(zp), dev_xm)
            self.send(8, self.b(zp), self.b(zp), dev_zm)

        def x_own(self):
            self.recv(4, self.fm(z))
            self.recv(5, self.fp(z))

        def wave2(self):
            self.recv(3, self.a(zp))
            self.send(10, self.a(zp), self.fm(zp), dev_xp)
            self.recv(1, self.b(zm))
            self.send(11, self.b(zm), self.fp(zm), dev_xm)

        def wave3(self):
            self.recv(6, self.a(z2))
            self.send(12, self.a(z2), self.fm(z2), dev_xp)
            self.recv(8, self.b(z2))
            self.send(13, self.b(z2), self.fp(z2), dev_xm)

        def x_near(self):
            self.recv(7, self.fm(zm))
            self.recv(9, self.fp(zp))
            self.recv(10, self.fm(zp))
            self.recv(11, self.fp(zm))

        def x_far(self):
            self.recv(12, self.fm(z2))
            self.recv(13, self.fp(z2))

    factor = 1.0 / math.sqrt(128)

    def head_norm(value, gain):
        meansq = jnp.mean(value * value, axis=-1, keepdims=True)
        return value * lax.rsqrt(meansq + 1e-06) * gain

    def project(g, pieces):
        rows = jnp.concatenate([mod[p] for p in pieces], axis=0)
        sums = jnp.dot(rows, w[...], preferred_element_type=F32)
        for h in range(3):
            qh = (head_norm(sums[:, h * 128:h * 128 + 128], qgain_ref[...]) * factor).astype(BF16)
            for i, p in enumerate(pieces):
                q[0, h, p] = qh[i * 32:i * 32 + 32]
            kh = head_norm(sums[:, 384 + h * 128:384 + h * 128 + 128], kgain_ref[...])
            kv[h, 0, g, 0] = kh.astype(BF16)
            vh = sums[:, 768 + h * 128:768 + h * 128 + 128]
            kv[h, 0, g, 1] = vh.T.astype(BF16)

    def o_send(h, g, k):
        slot, dev = ((3, dev_yp), (1, dev_ym), (4, dev_core))[k]
        send(kv.at[h, 0, g], kv.at[h, slot, g], o_ssem.at[k, h, g], o_rsem.at[k, h, g], dev)

    def o_recv(h, g, k):
        dst = kv.at[h, (3, 1, 4)[k], g]
        make(dst, dst, o_ssem.at[k, h, g], o_rsem.at[k, h, g], dev_yp).wait_recv()

    halves = (pl.ds(0, 2), pl.ds(2, 2))

    def f_send(h, k):
        src, dst, dev = (
            (kv.at[h, 3, halves[0]], kv.at[h, 2, halves[0]], dev_yp),
            (kv.at[h, 1, halves[1]], kv.at[h, 2, halves[1]], dev_ym),
            (kv.at[h, 3], kv.at[h, 7], dev_core),
            (kv.at[h, 1], kv.at[h, 5], dev_core),
            (kv.at[h, 2], kv.at[h, 6], dev_core),
        )[k]
        send(src, dst, f_ssem.at[h, k], f_rsem.at[h, k], dev)

    def f_recv(h, k):
        dst = (kv.at[h, 2, halves[0]], kv.at[h, 2, halves[1]], kv.at[h, 7], kv.at[h, 5], kv.at[h, 6])[k]
        make(dst, dst, f_ssem.at[h, k], f_rsem.at[h, k], dev_yp).wait_recv()

    def own_block(g):
        for h in range(3):
            for k in range(3):
                o_send(h, g, k)

    ga = Gather(
        lambda i: mod.at[i], lambda i: mod.at[12 + i], lambda i: mod.at[8 + i], lambda i: mod.at[4 + i],
        a_ssem, a_rsem,
    )
    ga.start()
    for c_ in w_copies:
        c_.wait()
    ga.wave1()
    ga.x_own()
    project(0, [z, 12 + z, 8 + z, 4 + z])
    own_block(0)
    ga.wave2()
    project(1, [zm, 12 + zm, zp, 12 + zp])
    own_block(1)
    ga.wave3()
    ga.x_near()
    project(2, [8 + zm, 4 + zm, 8 + zp, 4 + zp])
    own_block(2)
    ga.x_far()
    project(3, [z2, 12 + z2, 8 + z2, 4 + z2])
    for h in range(3):
        o_send(h, 3, 1)
        o_send(h, 3, 2)
        send(q.at[0, h], q.at[1, h], q_ssem.at[h], q_rsem.at[h], dev_x2)
    o_send(0, 3, 0)
    o_send(1, 3, 0)
    for h in range(3):
        o_recv(h, 0, 0)
        o_recv(h, 1, 0)
        f_send(h, 0)
        if h == 0:
            o_send(2, 3, 0)

    def near_y(h):
        for g in range(4):
            o_recv(h, g, 1)
        f_send(h, 1)
        f_send(h, 3)
        for g in (2, 3):
            o_recv(h, g, 0)
        f_send(h, 2)

    def far_y(h):
        f_recv(h, 0)
        f_recv(h, 1)
        f_send(h, 4)

    def sibling_near(h):
        f_recv(h, 2)
        f_recv(h, 3)

    def queries_in(h):
        make(q.at[1, h], q.at[1, h], q_ssem.at[h], q_rsem.at[h], dev_x2).wait_recv()

    def step_of(j):
        r = (j + 4) % 7
        h = jnp.where(j < 3, j, (j + 4) // 7 - 1)
        partner = jnp.where((r >= 1) & (r <= 4), 1, 0)
        dy = jnp.where((r == 4) | (r == 6), 2, jnp.where((r == 3) | (r == 5), 3, jnp.where(r == 1, 0, 1)))
        return h, jnp.where(j < 3, 0, partner), jnp.where(j < 3, 0, dy)

    def score(h, side, slot, buf):
        keys = jnp.concatenate([kv[h, slot, g, 0] for g in range(4)], axis=0)
        s_s[buf] = lax.dot_general(keys, q[side, h].reshape(512, 128), NT, preferred_element_type=F32)

    def soft(h, side, slot, buf):
        vals = jnp.concatenate([kv[h, slot, g, 1] for g in range(4)], axis=1)
        i = h * 2 + side
        scores = s_s[buf]
        old = m_s[i]
        new = jnp.maximum(old, jnp.max(scores, axis=0, keepdims=True))
        rescale = jnp.exp(old - new)
        powers = jnp.exp(scores - new)
        m_s[i] = new
        l_s[i] = l_s[i] * rescale + jnp.sum(powers, axis=0, keepdims=True)
        acc[i] = acc[i] * rescale + jnp.dot(vals, powers.astype(BF16), preferred_element_type=F32)

    def partner_done(h):
        i = h * 2 + 1
        osend[h] = (acc[i] / l_s[i]).astype(BF16)
        stsend[h, 0:1] = m_s[i]
        stsend[h, 1:2] = l_s[i]
        send(osend.at[h], orecv.at[h], e_ssem.at[0, h], e_rsem.at[0, h], dev_x2)
        send(stsend.at[h], strecv.at[h], e_ssem.at[1, h], e_rsem.at[1, h], dev_x2)

    def combine(h):
        i = h * 2
        make(orecv.at[h], orecv.at[h], e_ssem.at[0, h], e_rsem.at[0, h], dev_x2).wait_recv()
        make(strecv.at[h], strecv.at[h], e_ssem.at[1, h], e_rsem.at[1, h], dev_x2).wait_recv()
        other_m, other_l = strecv[h, 0:1], strecv[h, 1:2]
        top = jnp.maximum(m_s[i], other_m)
        mine = jnp.exp(m_s[i] - top)
        theirs = jnp.exp(other_m - top) * other_l
        inverse = 1.0 / (l_s[i] * mine + theirs)
        result = acc[i] * (mine * inverse) + orecv[h].astype(F32) * (theirs * inverse)
        result = result.T.astype(BF16)
        att[h, 0, z, 0] = result[:256]
        att[h, 0, z, 1] = result[256:]

    gathers = []
    for h in range(3):
        gc = Gather(
            lambda i, h=h: att.at[h, 0, i, 0], lambda i, h=h: att.at[h, 0, i, 1],
            lambda i, h=h: att.at[h, 1, i, 1], lambda i, h=h: att.at[h, 1, i, 0],
            c_ssem.at[h], c_rsem.at[h],
        )
        gathers.append(gc)

    m_s[...] = jnp.full_like(m_s, -1e30)
    l_s[...] = jnp.zeros_like(l_s)
    acc[...] = jnp.zeros_like(acc)
    for h in range(3):
        for g in range(4):
            o_recv(h, g, 2)
    score(0, 0, 0, 0)

    services = {}

    def service(j, *steps):
        services.setdefault(j, []).extend(steps)

    service(2, lambda: near_y(0))
    service(3, lambda: sibling_near(0), lambda: queries_in(0))
    service(4, lambda: near_y(1))
    service(6, lambda: far_y(0), lambda: near_y(2))
    service(7, lambda: f_recv(0, 4))
    service(8, lambda: partner_done(0))
    service(10, lambda: sibling_near(1), lambda: queries_in(1), lambda: far_y(1))
    service(14, lambda: f_recv(1, 4), lambda: combine(0), gathers[0].start)
    service(15, lambda: partner_done(1), lambda: far_y(2))
    service(17, lambda: sibling_near(2), lambda: queries_in(2))
    service(19, gathers[0].wave1, gathers[0].wave2)
    service(21, lambda: f_recv(2, 4), lambda: combine(1), gathers[1].start)
    service(22, lambda: partner_done(2), gathers[0].wave3)

    def body(j, carry):
        for at, steps in services.items():
            @pl.when(j == at)
            def _(steps=steps):
                for step in steps:
                    step()

        h, side, dy = step_of(j)
        h_, side_, dy_ = step_of(jnp.minimum(j + 1, 23))
        score(h, side, dy + 4, 1)
        soft(h, side, dy, 0)
        score(h_, side_, dy_, 0)
        soft(h, side, dy + 4, 1)
        return carry

    lax.fori_loop(0, 24, body, 0)
    gathers[1].wave1()
    gathers[1].wave2()
    combine(2)
    gathers[2].start()
    gathers[1].wave3()

    def project_out(h, first):
        def body(i, carry):
            z0 = i
            rows = jnp.concatenate(
                [att[h, c_, z0].reshape(512, 128) for c_ in range(2)], axis=1
            )
            weights = jnp.concatenate([wo[(xl * 4 + z0) * 3 + h], wo[((1 - xl) * 4 + z0) * 3 + h]], axis=0)
            oacc[...] += jnp.dot(rows, weights, preferred_element_type=F32)
            return carry

        lax.fori_loop(0, 4, body, 0)

    oacc[...] = jnp.zeros_like(oacc)
    for h in range(3):
        if h == 2:
            gathers[2].wave1()
            gathers[2].wave2()
            gathers[2].wave3()
        gathers[h].x_own()
        gathers[h].x_near()
        gathers[h].x_far()
        project_out(h, h == 0)

    outb[...] = oacc[...].astype(BF16).reshape(16, 32, 384)
    for d in range(4):
        zd = (z + d) % 4
        if d == 0:
            drec[0, u] = outb[z]
            drec[1, u] = outb[12 + z]
        else:
            dev = device(x, y, zd, core)
            send(outb.at[zd], drec.at[0, u], d_ssem.at[0, d], d_rsem.at[0, d], dev)
            send(outb.at[12 + zd], drec.at[1, u], d_ssem.at[1, d], d_rsem.at[1, d], dev)
        send(outb.at[8 + zd], drec.at[0, u], d_ssem.at[2, d], d_rsem.at[2, d], device(xm, y, zd, core))
        send(outb.at[4 + zd], drec.at[1, u], d_ssem.at[3, d], d_rsem.at[3, d], device(xp, y, zd, core))
    for d in range(4):
        zs = (z + 4 - d) % 4
        for kind in range(4):
            if d == 0 and kind < 2:
                continue
            dst = drec.at[kind % 2, (xl if kind < 2 else 1 - xl) * 4 + zs]
            make(dst, dst, d_ssem.at[kind, d], d_rsem.at[kind, d], dev_zp).wait_recv()
    for v in range(8):
        cols = pl.ds(v * 384, 384)
        branch = jnp.concatenate([drec[0, v], drec[1, v]], axis=0).astype(F32)
        out_ref[:, cols] = (tokens_ref[:, cols].astype(F32) + gate_ref[:, cols] * branch).astype(BF16)

    for gather in [ga] + gathers:
        for t in range(14):
            sent(gather.a(z), gather.ssem.at[t], gather.rsem.at[t])
    for h in range(3):
        for k in range(3):
            for g in range(4):
                sent(kv.at[h, 0, g], o_ssem.at[k, h, g], o_rsem.at[k, h, g])
        for k in range(5):
            sent(kv.at[h, 0, halves[0]] if k < 2 else kv.at[h, 0], f_ssem.at[h, k], f_rsem.at[h, k])
        sent(q.at[0, h], q_ssem.at[h], q_rsem.at[h])
        sent(osend.at[h], e_ssem.at[0, h], e_rsem.at[0, h])
        sent(stsend.at[h], e_ssem.at[1, h], e_rsem.at[1, h])
    for d in range(4):
        for kind in range(4):
            if d or kind > 1:
                sent(outb.at[0], d_ssem.at[kind, d], d_rsem.at[kind, d])


def local(tokens, mod_shift, mod_scale, mod_gate, qkv_weight, query_gain, key_gain, out_weight):
    vm = pl.BlockSpec(memory_space=pltpu.VMEM)
    anyspace = pl.BlockSpec(memory_space=pl.ANY)
    dma = pltpu.SemaphoreType.DMA
    return pl.pallas_call(
        kernel,
        out_shape=jax.ShapeDtypeStruct(tokens.shape, BF16),
        in_specs=[vm] * 6 + [anyspace] * 2,
        out_specs=vm,
        scratch_shapes=[
            pltpu.VMEM((3072, 1152), BF16),
            pltpu.VMEM((24, 128, 384), BF16),
            pltpu.VMEM((16, 32, 3072), BF16),
            pltpu.VMEM((2, 3, 16, 32, 128), BF16),
            pltpu.VMEM((3, 8, 4, 2, 128, 128), BF16),
            pltpu.VMEM((3, 2, 4, 2, 256, 128), BF16),
            pltpu.VMEM((16, 32, 384), BF16),
            pltpu.VMEM((2, 8, 32, 384), BF16),
            pltpu.VMEM((6, 1, 512), F32),
            pltpu.VMEM((6, 1, 512), F32),
            pltpu.VMEM((6, 128, 512), F32),
            pltpu.VMEM((2, 512, 512), F32),
            pltpu.VMEM((3, 128, 512), BF16),
            pltpu.VMEM((3, 128, 512), BF16),
            pltpu.VMEM((3, 8, 512), F32),
            pltpu.VMEM((3, 8, 512), F32),
            pltpu.VMEM((512, 384), F32),
            dma((4,)),
            dma((14,)), dma((14,)),
            dma((3, 3, 4)), dma((3, 3, 4)),
            dma((3, 5)), dma((3, 5)),
            dma((3,)), dma((3,)),
            dma((2, 3)), dma((2, 3)),
            dma((3, 14)), dma((3, 14)),
            dma((4, 4)), dma((4, 4)),
        ],
        compiler_params=pltpu.CompilerParams(
            collective_id=0, has_side_effects=True, vmem_limit_bytes=60 * 1024 * 1024
        ),
        name="joint_attention",
    )(
        tokens, mod_shift.reshape(1, -1), mod_scale.reshape(1, -1), mod_gate.reshape(1, -1),
        query_gain.reshape(1, -1), key_gain.reshape(1, -1), qkv_weight, out_weight.reshape(24, 128, 384),
    )


def solution(mesh):
    in_specs = (
        P(("blk", "ulysses"), None),
        P(),
        P(),
        P(),
        P(None, None, "ulysses"),
        P(),
        P(),
        P(None, "ulysses"),
    )
    out_specs = P(("blk", "ulysses"), None)
    return jax.shard_map(local, mesh=mesh, in_specs=in_specs, out_specs=out_specs, check_vma=False)
```

```python
import math

import jax
import jax.numpy as jnp
from jax import lax
from jax.experimental import pallas as pl
from jax.experimental.pallas import tpu as pltpu
from jax.sharding import PartitionSpec as P

MESH = pl.DeviceIdType.MESH
F32 = jnp.float32
BF16 = jnp.bfloat16
LOG2E = math.log2(math.e)


def kernel(
    tokens_ref, shift_ref, scale_ref, gate_ref, qgain_ref, kgain_ref, w_hbm, wo_hbm,
    out_ref,
    w, wo, mod, q, kv, att, outb, drec, m_s, l_s, acc, s_s, qt, osend, orecv, stsend, strecv, oacc,
    w_sem, s_sem, a_rsem, ob_rsem, f_rsem, q_rsem, e_rsem, c_rsem, d_rsem,
):
    blk = lax.axis_index("blk")
    u = lax.axis_index("ulysses")
    y, xh, core = blk // 4, (blk // 2) % 2, blk % 2
    xl, z = u // 4, u % 4
    x = xh * 2 + xl

    def device(x_, y_, z_, c_):
        return (y_ * 4 + (x_ // 2) * 2 + c_, (x_ % 2) * 4 + z_)

    zp, zm, z2 = (z + 1) % 4, (z + 3) % 4, (z + 2) % 4
    xp, xm, x2 = (x + 1) % 4, (x + 3) % 4, (x + 2) % 4
    yp, ym = (y + 1) % 4, (y + 3) % 4
    dev_zp, dev_zm = device(x, y, zp, core), device(x, y, zm, core)
    dev_xp, dev_xm = device(xp, y, z, core), device(xm, y, z, core)
    dev_x2 = device(x2, y, z, core)
    dev_z2 = device(x, y, z2, core)
    dev_yp, dev_ym = device(x, yp, z, core), device(x, ym, z, core)
    dev_core = device(x, y, z, 1 - core)

    barrier = pltpu.get_barrier_semaphore()
    partners = [dev_yp, dev_ym, dev_x2, dev_core]
    for d in range(4):
        zd = (z + d) % 4
        if d:
            partners.append(device(x, y, zd, core))
        partners.append(device(xp, y, zd, core))
        partners.append(device(xm, y, zd, core))
    for p in partners:
        pl.semaphore_signal(barrier, inc=1, device_id=p, device_id_type=MESH)

    w_copies = [
        pltpu.make_async_copy(w_hbm.at[j], w.at[:, pl.ds(j * 384, 384)], w_sem.at[j]) for j in range(3)
    ]
    w_copies.append(pltpu.make_async_copy(wo_hbm, wo, w_sem.at[3]))
    for c_ in w_copies:
        c_.start()

    wide = tokens_ref[...].astype(F32)
    center = jnp.mean(wide, axis=-1, keepdims=True)
    spread = jnp.mean((wide - center) ** 2, axis=-1, keepdims=True)
    normed = (wide - center) / jnp.sqrt(spread + 1e-06)
    modulated = (normed * (1.0 + scale_ref[...]) + shift_ref[...]).astype(BF16)
    mod[z] = modulated[:32]
    mod[12 + z] = modulated[32:]

    pl.semaphore_wait(barrier, len(partners))

    def make(src, dst, ssem, rsem, dev):
        return pltpu.make_async_remote_copy(
            src_ref=src, dst_ref=dst, send_sem=ssem, recv_sem=rsem, device_id=dev, device_id_type=MESH
        )

    def send(src, dst, ssem, rsem, dev):
        make(src, dst, ssem, rsem, dev).start()

    def arrived(dst, rsem):
        make(dst, dst, s_sem.at[0], rsem, dev_zp).wait_recv()

    class Gather:
        def __init__(self, own_a, own_b, from_minus, from_plus, ssem, rsem, slots=range(24)):
            self.a, self.b, self.fm, self.fp = own_a, own_b, from_minus, from_plus
            self.ssem, self.rsem, self.slots = ssem, rsem, slots

        def send(self, t, src, dst, dev):
            send(src, dst, self.ssem, self.rsem.at[self.slots[t]], dev)

        def recv(self, t, dst):
            arrived(dst, self.rsem.at[self.slots[t]])

        def start_split(self):
            for i in range(2):
                part = pl.ds(i * 16, 16)
                self.send(14 if i else 0, self.a(z).at[part], self.a(z).at[part], dev_zp)
                self.send(15 if i else 2, self.b(z).at[part], self.b(z).at[part], dev_zm)
            self.send(4, self.a(z), self.fm(z), dev_xp)
            self.send(5, self.b(z), self.fp(z), dev_xm)
            for i in range(2):
                part = pl.ds(i * 16, 16)
                self.send(18 if i else 1, self.b(z).at[part], self.b(z).at[part], dev_zp)
                self.send(19 if i else 3, self.a(z).at[part], self.a(z).at[part], dev_zm)

        def wave2_split(self):
            for i in range(2):
                part = pl.ds(i * 16, 16)
                self.recv(19 if i else 3, self.a(zp).at[part])
                self.send(20 if i else 10, self.a(zp).at[part], self.fm(zp).at[part], dev_xp)
                self.recv(18 if i else 1, self.b(zm).at[part])
                self.send(21 if i else 11, self.b(zm).at[part], self.fp(zm).at[part], dev_xm)

        def wave1_split(self):
            for i in range(2):
                part = pl.ds(i * 16, 16)
                self.recv(14 if i else 0, self.a(zm).at[part])
                self.send(16 if i else 7, self.a(zm).at[part], self.fm(zm).at[part], dev_xp)
                self.recv(15 if i else 2, self.b(zp).at[part])
                self.send(17 if i else 9, self.b(zp).at[part], self.fp(zp).at[part], dev_xm)
            self.send(6, self.a(zm), self.a(zm), dev_zp)
            self.send(8, self.b(zp), self.b(zp), dev_zm)

        def x_near_split(self):
            for i in range(2):
                part = pl.ds(i * 16, 16)
                self.recv(16 if i else 7, self.fm(zm).at[part])
                self.recv(17 if i else 9, self.fp(zp).at[part])
                self.recv(20 if i else 10, self.fm(zp).at[part])
                self.recv(21 if i else 11, self.fp(zm).at[part])

        def start(self):
            self.send(0, self.a(z), self.a(z), dev_zp)
            self.send(2, self.b(z), self.b(z), dev_zm)
            self.send(4, self.a(z), self.fm(z), dev_xp)
            self.send(5, self.b(z), self.fp(z), dev_xm)
            self.send(1, self.b(z), self.b(z), dev_zp)
            self.send(3, self.a(z), self.a(z), dev_zm)

        def wave1(self):
            self.recv(0, self.a(zm))
            self.send(7, self.a(zm), self.fm(zm), dev_xp)
            self.send(6, self.a(zm), self.a(zm), dev_zp)
            self.recv(2, self.b(zp))
            self.send(9, self.b(zp), self.fp(zp), dev_xm)
            self.send(8, self.b(zp), self.b(zp), dev_zm)

        def x_own(self):
            self.recv(4, self.fm(z))
            self.recv(5, self.fp(z))

        def wave2(self):
            self.recv(3, self.a(zp))
            self.send(10, self.a(zp), self.fm(zp), dev_xp)
            self.recv(1, self.b(zm))
            self.send(11, self.b(zm), self.fp(zm), dev_xm)

        def wave3(self):
            self.recv(7, self.fm(zm))
            self.send(12, self.fm(zm), self.fm(zm), dev_zp)
            self.recv(9, self.fp(zp))
            self.send(13, self.fp(zp), self.fp(zp), dev_zm)

        def wave3_split(self):
            part = pl.ds(16, 16)
            self.recv(16, self.fm(zm).at[part])
            self.send(22, self.fm(zm).at[part], self.fm(zm).at[part], dev_zp)
            self.recv(17, self.fp(zp).at[part])
            self.send(23, self.fp(zp).at[part], self.fp(zp).at[part], dev_zm)
            part = pl.ds(0, 16)
            self.recv(6, self.a(z2))
            self.send(12, self.a(z2).at[part], self.fm(z2).at[part], dev_xp)
            self.recv(8, self.b(z2))
            self.send(13, self.b(z2).at[part], self.fp(z2).at[part], dev_xm)

        def x_near_split(self):
            for i in range(2):
                part = pl.ds(i * 16, 16)
                if i == 0:
                    self.recv(7, self.fm(zm).at[part])
                    self.recv(9, self.fp(zp).at[part])
                self.recv(20 if i else 10, self.fm(zp).at[part])
                self.recv(21 if i else 11, self.fp(zm).at[part])

        def x_far_split(self):
            for i in range(2):
                part = pl.ds(i * 16, 16)
                self.recv(22 if i else 12, self.fm(z2).at[part])
                self.recv(23 if i else 13, self.fp(z2).at[part])

    factor = 1.0 / math.sqrt(128)

    def head_norm(value, gain):
        meansq = jnp.mean(value * value, axis=-1, keepdims=True)
        return value * lax.rsqrt(meansq + 1e-06) * gain

    def project(g, pieces):
        rows = jnp.concatenate([mod[p] for p in pieces], axis=0)
        sums = jnp.dot(rows, w[...], preferred_element_type=F32)
        for h in range(3):
            qh = (head_norm(sums[:, h * 128:h * 128 + 128], qgain_ref[...]) * factor).astype(BF16)
            for i, p in enumerate(pieces):
                q[0, h, p] = qh[i * 32:i * 32 + 32]
            kh = head_norm(sums[:, 384 + h * 128:384 + h * 128 + 128], kgain_ref[...])
            kv[h, 0, g, 0] = kh.astype(BF16)
            vh = sums[:, 768 + h * 128:768 + h * 128 + 128]
            kv[h, 0, g, 1] = vh.T.astype(BF16)

    def o_send(h, g, k):
        slot, dev = ((3, dev_yp), (1, dev_ym), (4, dev_core))[k]
        sem = (1 + h if g else 0, 4 + h, 7)[k]
        send(kv.at[h, 0, g], kv.at[h, slot, g], s_sem.at[1], ob_rsem.at[sem], dev)

    def f_send(h, k):
        if k < 4:
            src, dst, dev = kv.at[h, 1 if k % 2 else 3, k], kv.at[h, 2, k], dev_ym if k % 2 else dev_yp
        else:
            slot = (3, 1, 2)[k - 4]
            src, dst, dev = kv.at[h, slot], kv.at[h, slot + 4], dev_core
        send(src, dst, s_sem.at[1], f_rsem.at[h, max(k - 3, 0)], dev)

    def f_recv(h, k):
        arrived(kv.at[h, (7, 5, 6)[k - 4]], f_rsem.at[h, k - 3])

    def own_block(g, heads=(0, 1, 2)):
        for h in heads:
            for k in range(3):
                o_send(h, g, k)

    ga = Gather(
        lambda i: mod.at[i], lambda i: mod.at[12 + i], lambda i: mod.at[8 + i], lambda i: mod.at[4 + i],
        s_sem.at[0], a_rsem,
    )
    ga.start_split()
    ga.wave1_split()
    ga.x_own()
    for c_ in w_copies[:3]:
        c_.wait()
    project(0, [z, 12 + z, 8 + z, 4 + z])
    own_block(0)
    ga.wave2_split()
    project(1, [zm, 12 + zm, zp, 12 + zp])
    own_block(1)
    ga.wave3_split()
    ga.x_near_split()
    project(2, [8 + zm, 4 + zm, 8 + zp, 4 + zp])
    arrived(kv.at[:, 3, 0], ob_rsem.at[0])
    f_send(0, 0)
    own_block(2)
    ga.x_far_split()
    project(3, [z2, 12 + z2, 8 + z2, 4 + z2])
    for h in range(3):
        if h < 2:
            o_send(h, 3, 0)
            o_send(h, 3, 1)
        o_send(h, 3, 2)
        send(q.at[0, h], q.at[1, h], s_sem.at[2], q_rsem.at[h], dev_x2)

    def near_y(h):
        if h:
            f_send(h, 0)
        arrived(kv.at[h, 1], ob_rsem.at[4 + h])
        f_send(h, 1)
        f_send(h, 3)
        f_send(h, 5)
        arrived(kv.at[h, 3, pl.ds(1, 3)], ob_rsem.at[1 + h])
        f_send(h, 2)
        f_send(h, 4)

    def far_y(h):
        arrived(kv.at[h, 2], f_rsem.at[h, 0])
        f_send(h, 6)

    def sibling_near(h):
        f_recv(h, 4)
        f_recv(h, 5)

    def queries_in(h):
        arrived(q.at[1, h], q_rsem.at[h])
        split_queries(h, 1)

    own_keys, near_keys, sibling_keys, far_keys = range(4)
    order = [(0, 0, own_keys), (1, 0, own_keys), (2, 0, own_keys), (0, 0, near_keys)]
    order += [(1, 0, near_keys), (0, 1, own_keys), (0, 1, near_keys), (0, 1, sibling_keys)]
    order += [(0, 0, sibling_keys), (1, 0, sibling_keys), (0, 1, far_keys), (0, 0, far_keys)]
    order += [(1, 1, own_keys), (1, 1, near_keys), (1, 1, sibling_keys), (2, 1, own_keys)]
    order += [(1, 1, far_keys), (2, 1, near_keys), (1, 0, far_keys), (2, 1, sibling_keys)]
    order += [(2, 1, far_keys), (2, 0, near_keys), (2, 0, sibling_keys), (2, 0, far_keys)]
    codes = [(h * 2 + side) * 4 + k for h, side, k in order]
    words = [sum(c << (5 * n) for n, c in enumerate(codes[w * 6:w * 6 + 6])) for w in range(4)]

    def step_of(j):
        w = j // 6
        word = jnp.where(w < 2, jnp.where(w < 1, words[0], words[1]), jnp.where(w < 3, words[2], words[3]))
        code = jnp.right_shift(word, 5 * (j % 6)) % 32
        i, k = code // 4, code % 4
        return i // 2, i % 2, k + 3 * (k // 2) - 4 * (k // 3), 4 - k + 5 * (k // 2)

    def split_queries(h, side):
        wide_q = q[side, h].reshape(512, 128).astype(F32) * LOG2E
        high = wide_q.astype(BF16)
        low = (wide_q - high.astype(F32)).astype(BF16)
        qt[h * 2 + side] = jnp.concatenate([high, low], axis=1).T

    def score(h, side, slot, buf):
        keys = jnp.concatenate([kv[h, slot, g, 0] for g in range(4)], axis=0)
        keys = jnp.concatenate([keys, keys], axis=1)
        s_s[buf] = jnp.dot(keys, qt[h * 2 + side], preferred_element_type=F32)

    def soft(h, side, slot, buf):
        vals = jnp.concatenate([kv[h, slot, g, 1] for g in range(4)], axis=1)
        i = h * 2 + side
        scores = s_s[buf]
        old = m_s[i]
        new = jnp.maximum(old, jnp.max(scores, axis=0, keepdims=True))
        rescale = jnp.exp2(old - new)
        powers = jnp.exp2(scores - new)
        m_s[i] = new
        l_s[i] = l_s[i] * rescale + jnp.sum(powers, axis=0, keepdims=True)
        acc[i] = acc[i] * rescale + jnp.dot(vals, powers.astype(BF16), preferred_element_type=F32)

    def partner_done(h):
        i = h * 2 + 1
        osend[h] = (acc[i] / l_s[i]).astype(BF16)
        stsend[h, 0:1] = m_s[i]
        stsend[h, 1:2] = l_s[i]
        send(osend.at[h], orecv.at[h], s_sem.at[3], e_rsem.at[0, h], dev_x2)
        send(stsend.at[h], strecv.at[h], s_sem.at[4], e_rsem.at[1, h], dev_x2)

    def combine(h):
        i = h * 2
        arrived(orecv.at[h], e_rsem.at[0, h])
        arrived(strecv.at[h], e_rsem.at[1, h])
        other_m, other_l = strecv[h, 0:1], strecv[h, 1:2]
        top = jnp.maximum(m_s[i], other_m)
        mine = jnp.exp2(m_s[i] - top)
        theirs = jnp.exp2(other_m - top) * other_l
        inverse = 1.0 / (l_s[i] * mine + theirs)
        result = acc[i] * (mine * inverse) + orecv[h].astype(F32) * (theirs * inverse)
        result = result.T.astype(BF16)
        att[h, 0, z, 0] = result[:256]
        att[h, 0, z, 1] = result[256:]

    gathers = []
    for h in range(3):
        gc = Gather(
            lambda i, h=h: att.at[h, 0, i, 0], lambda i, h=h: att.at[h, 0, i, 1],
            lambda i, h=h: att.at[h, 1, i, 1], lambda i, h=h: att.at[h, 1, i, 0],
            s_sem.at[5], c_rsem.at[h], (0, 1, 2, 3, 6, 6, 6, 4, 6, 5, 6, 6, 6, 6),
        )
        gathers.append(gc)

    for h in range(3):
        split_queries(h, 0)
    m_s[...] = jnp.full_like(m_s, -1e30)
    l_s[...] = jnp.zeros_like(l_s)
    acc[...] = jnp.zeros_like(acc)
    arrived(kv.at[:, 4], ob_rsem.at[7])
    score(0, 0, 0, 0)

    services = {}

    def service(j, *steps):
        services.setdefault(j, []).extend(steps)

    def last_own():
        o_send(2, 3, 0)
        o_send(2, 3, 1)

    service(1, lambda: near_y(0), last_own, lambda: near_y(1))
    service(2, lambda: queries_in(0))
    service(3, lambda: sibling_near(0), lambda: sibling_near(1))
    service(4, lambda: far_y(0))
    service(5, lambda: f_recv(0, 6), lambda: queries_in(1), lambda: near_y(2))
    service(6, lambda: partner_done(0), lambda: queries_in(2))
    service(7, lambda: far_y(1))
    service(8, lambda: f_recv(1, 6), lambda: sibling_near(2))
    service(9, lambda: partner_done(1), lambda: far_y(2))
    service(10, lambda: f_recv(2, 6), lambda: combine(0), gathers[0].start)
    service(11, lambda: partner_done(2))

    def dispatch(i, keys):
        if len(keys) == 1:
            for step in services[keys[0]]:
                step()
            return
        middle = len(keys) // 2
        pl.when(i < keys[middle])(lambda: dispatch(i, keys[:middle]))
        pl.when(i >= keys[middle])(lambda: dispatch(i, keys[middle:]))

    for i in range(12):
        services.setdefault(i, [])

    def body(i, carry):
        dispatch(i, sorted(services))
        j = i * 2
        at = [step_of(j), step_of(j + 1), step_of(jnp.minimum(j + 2, 23))]
        for n in range(2):
            (h, side, even, odd), (h_, side_, even_, _) = at[n], at[n + 1]
            score(h, side, odd, 1)
            soft(h, side, even, 0)
            score(h_, side_, even_, 0)
            soft(h, side, odd, 1)
        return carry

    lax.fori_loop(0, 12, body, 0)

    def gathered(h):
        arrived(att.at[h, 0], c_rsem.at[h, 6])

    def project_out(h):
        rows = jnp.concatenate(
            [att[h, c_, z0].reshape(512, 128) for c_ in range(2) for z0 in range(4)], axis=1
        )
        weights = jnp.concatenate(
            [wo[((xl + c_) % 2 * 4 + z0) * 3 + h] for c_ in range(2) for z0 in range(4)], axis=0
        )
        total = jnp.dot(rows, weights, preferred_element_type=F32)
        oacc[...] = total if h == 0 else oacc[...] + total

    combine(1)
    gathers[1].start()
    gathers[0].wave1()
    gathers[0].wave2()
    w_copies[3].wait()
    combine(2)
    gathers[2].start()
    gathers[1].wave1()
    gathers[0].wave3()
    gathers[1].wave2()
    gathers[2].wave1()
    gathers[1].wave3()
    gathers[2].wave2()
    gathered(0)
    project_out(0)
    gathers[2].wave3()
    gathered(1)
    project_out(1)
    gathered(2)
    project_out(2)

    outb[...] = oacc[...].astype(BF16).reshape(16, 32, 384)
    for d in range(4):
        zd = (z + d) % 4
        if d == 0:
            drec[0, u] = outb[z]
            drec[1, u] = outb[12 + z]
        else:
            dev = device(x, y, zd, core)
            send(outb.at[zd], drec.at[0, u], s_sem.at[6], d_rsem.at[0], dev)
            send(outb.at[12 + zd], drec.at[1, u], s_sem.at[6], d_rsem.at[0], dev)
        send(outb.at[8 + zd], drec.at[0, u], s_sem.at[6], d_rsem.at[0], device(xm, y, zd, core))
        send(outb.at[4 + zd], drec.at[1, u], s_sem.at[6], d_rsem.at[0], device(xp, y, zd, core))
    arrived(outb.at[pl.ds(0, 14)], d_rsem.at[0])
    for v in range(8):
        cols = pl.ds(v * 384, 384)
        branch = jnp.concatenate([drec[0, v], drec[1, v]], axis=0).astype(F32)
        out_ref[:, cols] = (tokens_ref[:, cols].astype(F32) + gate_ref[:, cols] * branch).astype(BF16)

    for n, group in enumerate((
        mod.at[pl.ds(0, 14)], kv.at[:, pl.ds(0, 7)], q.at[0], osend, stsend,
        kv.at[:, pl.ds(0, 7), pl.ds(0, 2)], outb.at[pl.ds(0, 14)],
    )):
        make(group, group, s_sem.at[n], d_rsem.at[0], dev_zp).wait_send()


def local(tokens, mod_shift, mod_scale, mod_gate, qkv_weight, query_gain, key_gain, out_weight):
    vm = pl.BlockSpec(memory_space=pltpu.VMEM)
    anyspace = pl.BlockSpec(memory_space=pl.ANY)
    dma = pltpu.SemaphoreType.DMA
    return pl.pallas_call(
        kernel,
        out_shape=jax.ShapeDtypeStruct(tokens.shape, BF16),
        in_specs=[vm] * 6 + [anyspace] * 2,
        out_specs=vm,
        scratch_shapes=[
            pltpu.VMEM((3072, 1152), BF16),
            pltpu.VMEM((24, 128, 384), BF16),
            pltpu.VMEM((16, 32, 3072), BF16),
            pltpu.VMEM((2, 3, 16, 32, 128), BF16),
            pltpu.VMEM((3, 8, 4, 2, 128, 128), BF16),
            pltpu.VMEM((3, 2, 4, 2, 256, 128), BF16),
            pltpu.VMEM((16, 32, 384), BF16),
            pltpu.VMEM((2, 8, 32, 384), BF16),
            pltpu.VMEM((6, 1, 512), F32),
            pltpu.VMEM((6, 1, 512), F32),
            pltpu.VMEM((6, 128, 512), F32),
            pltpu.VMEM((2, 512, 512), F32),
            pltpu.VMEM((6, 256, 512), BF16),
            pltpu.VMEM((3, 128, 512), BF16),
            pltpu.VMEM((3, 128, 512), BF16),
            pltpu.VMEM((3, 8, 512), F32),
            pltpu.VMEM((3, 8, 512), F32),
            pltpu.VMEM((512, 384), F32),
            dma((4,)),
            dma((7,)),
            dma((24,)),
            dma((8,)),
            dma((3, 4)),
            dma((3,)),
            dma((2, 3)),
            dma((3, 7)),
            dma((1,)),
        ],
        compiler_params=pltpu.CompilerParams(
            collective_id=0, has_side_effects=True, vmem_limit_bytes=60 * 1024 * 1024
        ),
        name="joint_attention",
    )(
        tokens, mod_shift.reshape(1, -1), mod_scale.reshape(1, -1), mod_gate.reshape(1, -1),
        query_gain.reshape(1, -1), key_gain.reshape(1, -1), qkv_weight, out_weight.reshape(24, 128, 384),
    )


def solution(mesh):
    in_specs = (
        P(("blk", "ulysses"), None),
        P(),
        P(),
        P(),
        P(None, None, "ulysses"),
        P(),
        P(),
        P(None, "ulysses"),
    )
    out_specs = P(("blk", "ulysses"), None)
    return jax.shard_map(local, mesh=mesh, in_specs=in_specs, out_specs=out_specs, check_vma=False)
```

```python
import math

import jax
import jax.numpy as jnp
from jax import lax
from jax.experimental import pallas as pl
from jax.experimental.pallas import tpu as pltpu
from jax.sharding import PartitionSpec as P

MESH = pl.DeviceIdType.MESH
F32 = jnp.float32
BF16 = jnp.bfloat16
LOG2E = math.log2(math.e)


def kernel(
    tokens_ref, shift_ref, scale_ref, qgain_ref, kgain_ref, w_hbm, wo_hbm,
    out_ref,
    w, wo, mod, q, kv, att, outb, drec, m_s, l_s, acc, s_s, qt, osend, orecv, stsend, strecv, oacc,
    w_sem, s_sem, a_rsem, ob_rsem, f_rsem, q_rsem, e_rsem, c_rsem, d_rsem,
):
    blk = lax.axis_index("blk")
    u = lax.axis_index("ulysses")
    y, xh, core = blk // 4, (blk // 2) % 2, blk % 2
    xl, z = u // 4, u % 4
    x = xh * 2 + xl

    def device(x_, y_, z_, c_):
        return (y_ * 4 + (x_ // 2) * 2 + c_, (x_ % 2) * 4 + z_)

    zp, zm, z2 = (z + 1) % 4, (z + 3) % 4, (z + 2) % 4
    xp, xm, x2 = (x + 1) % 4, (x + 3) % 4, (x + 2) % 4
    yp, ym = (y + 1) % 4, (y + 3) % 4
    dev_zp, dev_zm = device(x, y, zp, core), device(x, y, zm, core)
    dev_xp, dev_xm = device(xp, y, z, core), device(xm, y, z, core)
    dev_x2 = device(x2, y, z, core)
    dev_z2 = device(x, y, z2, core)
    dev_yp, dev_ym = device(x, yp, z, core), device(x, ym, z, core)
    dev_core = device(x, y, z, 1 - core)

    barrier = pltpu.get_barrier_semaphore()
    partners = [dev_yp, dev_ym, dev_x2, dev_core]
    for d in range(4):
        zd = (z + d) % 4
        if d:
            partners.append(device(x, y, zd, core))
        partners.append(device(xp, y, zd, core))
        partners.append(device(xm, y, zd, core))
    for p in partners:
        pl.semaphore_signal(barrier, inc=1, device_id=p, device_id_type=MESH)

    w_copies = [
        pltpu.make_async_copy(w_hbm.at[j], w.at[:, pl.ds(j * 384, 384)], w_sem.at[j]) for j in range(3)
    ]
    w_copies.append(pltpu.make_async_copy(wo_hbm, wo, w_sem.at[3]))
    for c_ in w_copies:
        c_.start()

    wide = tokens_ref[...].astype(F32)
    center = jnp.mean(wide, axis=-1, keepdims=True)
    spread = jnp.mean((wide - center) ** 2, axis=-1, keepdims=True)
    normed = (wide - center) / jnp.sqrt(spread + 1e-06)
    modulated = (normed * (1.0 + scale_ref[...]) + shift_ref[...]).astype(BF16)
    mod[z] = modulated[:32]
    mod[12 + z] = modulated[32:]

    pl.semaphore_wait(barrier, len(partners))

    def make(src, dst, ssem, rsem, dev):
        return pltpu.make_async_remote_copy(
            src_ref=src, dst_ref=dst, send_sem=ssem, recv_sem=rsem, device_id=dev, device_id_type=MESH
        )

    def send(src, dst, ssem, rsem, dev):
        make(src, dst, ssem, rsem, dev).start()

    def arrived(dst, rsem):
        make(dst, dst, s_sem.at[0], rsem, dev_zp).wait_recv()

    class Gather:
        def __init__(self, own_a, own_b, from_minus, from_plus, ssem, rsem, slots=range(24)):
            self.a, self.b, self.fm, self.fp = own_a, own_b, from_minus, from_plus
            self.ssem, self.rsem, self.slots = ssem, rsem, slots

        def send(self, t, src, dst, dev):
            send(src, dst, self.ssem, self.rsem.at[self.slots[t]], dev)

        def recv(self, t, dst):
            arrived(dst, self.rsem.at[self.slots[t]])

        def start_split(self):
            for i in range(2):
                part = pl.ds(i * 16, 16)
                self.send(14 if i else 0, self.a(z).at[part], self.a(z).at[part], dev_zp)
                self.send(15 if i else 2, self.b(z).at[part], self.b(z).at[part], dev_zm)
            self.send(4, self.a(z), self.fm(z), dev_xp)
            self.send(5, self.b(z), self.fp(z), dev_xm)
            for i in range(2):
                part = pl.ds(i * 16, 16)
                self.send(18 if i else 1, self.b(z).at[part], self.b(z).at[part], dev_zp)
                self.send(19 if i else 3, self.a(z).at[part], self.a(z).at[part], dev_zm)

        def wave2_split(self):
            for i in range(2):
                part = pl.ds(i * 16, 16)
                self.recv(19 if i else 3, self.a(zp).at[part])
                self.send(20 if i else 10, self.a(zp).at[part], self.fm(zp).at[part], dev_xp)
                self.recv(18 if i else 1, self.b(zm).at[part])
                self.send(21 if i else 11, self.b(zm).at[part], self.fp(zm).at[part], dev_xm)

        def wave1_split(self):
            for i in range(2):
                part = pl.ds(i * 16, 16)
                self.recv(14 if i else 0, self.a(zm).at[part])
                self.send(16 if i else 7, self.a(zm).at[part], self.fm(zm).at[part], dev_xp)
                self.recv(15 if i else 2, self.b(zp).at[part])
                self.send(17 if i else 9, self.b(zp).at[part], self.fp(zp).at[part], dev_xm)
            self.send(6, self.a(zm), self.a(zm), dev_zp)
            self.send(8, self.b(zp), self.b(zp), dev_zm)

        def x_near_split(self):
            for i in range(2):
                part = pl.ds(i * 16, 16)
                self.recv(16 if i else 7, self.fm(zm).at[part])
                self.recv(17 if i else 9, self.fp(zp).at[part])
                self.recv(20 if i else 10, self.fm(zp).at[part])
                self.recv(21 if i else 11, self.fp(zm).at[part])

        def start(self):
            self.send(0, self.a(z), self.a(z), dev_zp)
            self.send(2, self.b(z), self.b(z), dev_zm)
            self.send(1, self.b(z), self.b(z), dev_zp)
            self.send(3, self.a(z), self.a(z), dev_zm)

        def far(self):
            self.send(6, self.a(z), self.a(z), dev_z2)
            self.send(8, self.b(z), self.b(z), dev_z2)

        def near(self):
            self.recv(0, self.a(zm))
            self.send(7, self.a(zm), self.fm(zm), dev_xp)
            self.recv(2, self.b(zp))
            self.send(9, self.b(zp), self.fp(zp), dev_xm)

        def cross(self):
            self.send(4, self.a(z), self.fm(z), dev_xp)
            self.send(5, self.b(z), self.fp(z), dev_xm)

        def wave3_x(self):
            self.recv(6, self.a(z2))
            self.send(12, self.a(z2), self.fm(z2), dev_xp)
            self.recv(8, self.b(z2))
            self.send(13, self.b(z2), self.fp(z2), dev_xm)

        def wave1(self):
            self.recv(0, self.a(zm))
            self.send(7, self.a(zm), self.fm(zm), dev_xp)
            self.send(6, self.a(zm), self.a(zm), dev_zp)
            self.recv(2, self.b(zp))
            self.send(9, self.b(zp), self.fp(zp), dev_xm)
            self.send(8, self.b(zp), self.b(zp), dev_zm)

        def x_own(self):
            self.recv(4, self.fm(z))
            self.recv(5, self.fp(z))

        def wave2(self):
            self.recv(3, self.a(zp))
            self.send(10, self.a(zp), self.fm(zp), dev_xp)
            self.recv(1, self.b(zm))
            self.send(11, self.b(zm), self.fp(zm), dev_xm)

        def wave3(self):
            self.recv(7, self.fm(zm))
            self.send(12, self.fm(zm), self.fm(zm), dev_zp)
            self.recv(9, self.fp(zp))
            self.send(13, self.fp(zp), self.fp(zp), dev_zm)

        def wave3_split(self):
            part = pl.ds(16, 16)
            self.recv(16, self.fm(zm).at[part])
            self.send(22, self.fm(zm).at[part], self.fm(zm).at[part], dev_zp)
            self.recv(17, self.fp(zp).at[part])
            self.send(23, self.fp(zp).at[part], self.fp(zp).at[part], dev_zm)
            part = pl.ds(0, 16)
            self.recv(6, self.a(z2))
            self.send(12, self.a(z2).at[part], self.fm(z2).at[part], dev_xp)
            self.recv(8, self.b(z2))
            self.send(13, self.b(z2).at[part], self.fp(z2).at[part], dev_xm)

        def x_near_split(self):
            for i in range(2):
                part = pl.ds(i * 16, 16)
                if i == 0:
                    self.recv(7, self.fm(zm).at[part])
                    self.recv(9, self.fp(zp).at[part])
                self.recv(20 if i else 10, self.fm(zp).at[part])
                self.recv(21 if i else 11, self.fp(zm).at[part])

        def x_far_split(self):
            for i in range(2):
                part = pl.ds(i * 16, 16)
                self.recv(22 if i else 12, self.fm(z2).at[part])
                self.recv(23 if i else 13, self.fp(z2).at[part])

    factor = 1.0 / math.sqrt(128)

    def head_norm(value, gain):
        meansq = jnp.mean(value * value, axis=-1, keepdims=True)
        return value * lax.rsqrt(meansq + 1e-06) * gain

    def project(g, pieces):
        rows = jnp.concatenate([mod[p] for p in pieces], axis=0)
        sums = jnp.dot(rows, w[...], preferred_element_type=F32)
        for h in range(3):
            qh = (head_norm(sums[:, h * 128:h * 128 + 128], qgain_ref[...]) * factor).astype(BF16)
            for i, p in enumerate(pieces):
                q[0, h, p] = qh[i * 32:i * 32 + 32]
            kh = head_norm(sums[:, 384 + h * 128:384 + h * 128 + 128], kgain_ref[...])
            kv[h, 0, g, 0] = kh.astype(BF16)
            vh = sums[:, 768 + h * 128:768 + h * 128 + 128]
            kv[h, 0, g, 1] = vh.T.astype(BF16)

    def o_send(h, g, k):
        slot, dev = ((3, dev_yp), (1, dev_ym), (4, dev_core))[k]
        sem = (1 + h if g else 0, 4 + h, 7)[k]
        send(kv.at[h, 0, g], kv.at[h, slot, g], s_sem.at[1], ob_rsem.at[sem], dev)

    def f_send(h, k):
        if k < 4:
            src, dst, dev = kv.at[h, 1 if k % 2 else 3, k], kv.at[h, 2, k], dev_ym if k % 2 else dev_yp
        else:
            slot = (3, 1, 2)[k - 4]
            src, dst, dev = kv.at[h, slot], kv.at[h, slot + 4], dev_core
        send(src, dst, s_sem.at[1], f_rsem.at[h, max(k - 3, 0)], dev)

    def f_recv(h, k):
        arrived(kv.at[h, (7, 5, 6)[k - 4]], f_rsem.at[h, k - 3])

    def own_block(g, heads=(0, 1, 2)):
        for h in heads:
            for k in range(3):
                o_send(h, g, k)

    ga = Gather(
        lambda i: mod.at[i], lambda i: mod.at[12 + i], lambda i: mod.at[8 + i], lambda i: mod.at[4 + i],
        s_sem.at[0], a_rsem,
    )
    ga.start_split()
    ga.wave1_split()
    ga.x_own()
    for c_ in w_copies[:3]:
        c_.wait()
    project(0, [z, 12 + z, 8 + z, 4 + z])
    own_block(0)
    ga.wave2_split()
    project(1, [zm, 12 + zm, zp, 12 + zp])
    own_block(1)
    ga.wave3_split()
    ga.x_near_split()
    project(2, [8 + zm, 4 + zm, 8 + zp, 4 + zp])
    arrived(kv.at[:, 3, 0], ob_rsem.at[0])
    f_send(0, 0)
    own_block(2)
    ga.x_far_split()
    project(3, [z2, 12 + z2, 8 + z2, 4 + z2])
    for h in range(3):
        o_send(h, 3, 2)
    for h in range(3):
        if h < 2:
            o_send(h, 3, 0)
            o_send(h, 3, 1)
        send(q.at[0, h], q.at[1, h], s_sem.at[2], q_rsem.at[h], dev_x2)

    def near_y(h):
        if h:
            f_send(h, 0)
        arrived(kv.at[h, 1], ob_rsem.at[4 + h])
        f_send(h, 1)
        f_send(h, 3)
        f_send(h, 5)
        arrived(kv.at[h, 3, pl.ds(1, 3)], ob_rsem.at[1 + h])
        f_send(h, 2)
        f_send(h, 4)

    def far_y(h):
        arrived(kv.at[h, 2], f_rsem.at[h, 0])
        f_send(h, 6)

    def sibling_near(h):
        f_recv(h, 4)
        f_recv(h, 5)

    def queries_in(h):
        arrived(q.at[1, h], q_rsem.at[h])
        split_queries(h, 1)

    own_keys, near_keys, sibling_keys, far_keys = range(4)
    order = [(0, 0, own_keys), (1, 0, own_keys), (2, 0, own_keys), (0, 0, near_keys)]
    order += [(1, 0, near_keys), (0, 1, own_keys), (0, 1, near_keys), (0, 1, sibling_keys)]
    order += [(0, 0, sibling_keys), (1, 0, sibling_keys), (0, 1, far_keys), (0, 0, far_keys)]
    order += [(1, 1, own_keys), (1, 1, near_keys), (1, 1, sibling_keys), (1, 1, far_keys)]
    order += [(2, 1, own_keys), (2, 1, near_keys), (2, 1, sibling_keys), (2, 1, far_keys)]
    order += [(1, 0, far_keys), (2, 0, near_keys), (2, 0, sibling_keys), (2, 0, far_keys)]
    codes = [(h * 2 + side) * 4 + k for h, side, k in order]
    words = [sum(c << (5 * n) for n, c in enumerate(codes[w * 6:w * 6 + 6])) for w in range(4)]

    def step_of(j):
        w = j // 6
        word = jnp.where(w < 2, jnp.where(w < 1, words[0], words[1]), jnp.where(w < 3, words[2], words[3]))
        code = jnp.right_shift(word, 5 * (j % 6)) % 32
        i, k = code // 4, code % 4
        return i // 2, i % 2, k + 3 * (k // 2) - 4 * (k // 3), 4 - k + 5 * (k // 2)

    def split_queries(h, side):
        wide_q = q[side, h].reshape(512, 128).astype(F32) * LOG2E
        high = wide_q.astype(BF16)
        low = (wide_q - high.astype(F32)).astype(BF16)
        qt[h * 2 + side] = jnp.concatenate([high, low], axis=1).T

    def score(h, side, slot, buf):
        keys = jnp.concatenate([kv[h, slot, g, 0] for g in range(4)], axis=0)
        keys = jnp.concatenate([keys, keys], axis=1)
        s_s[buf] = jnp.dot(keys, qt[h * 2 + side], preferred_element_type=F32)

    def soft(h, side, slot, buf):
        vals = jnp.concatenate([kv[h, slot, g, 1] for g in range(4)], axis=1)
        i = h * 2 + side
        scores = s_s[buf]
        old = m_s[i]
        new = jnp.maximum(old, jnp.max(scores, axis=0, keepdims=True))
        rescale = jnp.exp2(old - new)
        powers = jnp.exp2(scores - new)
        m_s[i] = new
        l_s[i] = l_s[i] * rescale + jnp.sum(powers, axis=0, keepdims=True)
        acc[i] = acc[i] * rescale + jnp.dot(vals, powers.astype(BF16), preferred_element_type=F32)

    def partner_done(h):
        i = h * 2 + 1
        osend[h] = (acc[i] / l_s[i]).astype(BF16)
        stsend[h, 0:1] = m_s[i]
        stsend[h, 1:2] = l_s[i]
        send(osend.at[h], orecv.at[h], s_sem.at[3], e_rsem.at[0, h], dev_x2)
        send(stsend.at[h], strecv.at[h], s_sem.at[4], e_rsem.at[1, h], dev_x2)

    def combine(h):
        i = h * 2
        arrived(orecv.at[h], e_rsem.at[0, h])
        arrived(strecv.at[h], e_rsem.at[1, h])
        other_m, other_l = strecv[h, 0:1], strecv[h, 1:2]
        top = jnp.maximum(m_s[i], other_m)
        mine = jnp.exp2(m_s[i] - top)
        theirs = jnp.exp2(other_m - top) * other_l
        inverse = 1.0 / (l_s[i] * mine + theirs)
        result = acc[i] * (mine * inverse) + orecv[h].astype(F32) * (theirs * inverse)
        result = result.T.astype(BF16)
        att[h, 0, z, 0] = result[:256]
        att[h, 0, z, 1] = result[256:]

    gathers = []
    for h in range(3):
        gc = Gather(
            lambda i, h=h: att.at[h, 0, i, 0], lambda i, h=h: att.at[h, 0, i, 1],
            lambda i, h=h: att.at[h, 1, i, 1], lambda i, h=h: att.at[h, 1, i, 0],
            s_sem.at[5], c_rsem.at[h],
            (0, 1, 2, 3, 6, 6, 4, 6, 5, 6, 6, 6, 6, 6) if h == 2 else (0, 1, 2, 3, 6, 6, 6, 4, 6, 5, 6, 6, 6, 6),
        )
        gathers.append(gc)

    for h in range(3):
        split_queries(h, 0)
    m_s[...] = jnp.full_like(m_s, -1e30)
    l_s[...] = jnp.zeros_like(l_s)
    acc[...] = jnp.zeros_like(acc)
    score(0, 0, 0, 0)
    arrived(kv.at[:, 4], ob_rsem.at[7])

    services = {}

    def service(j, *steps):
        services.setdefault(j, []).extend(steps)

    def last_own():
        o_send(2, 3, 0)
        o_send(2, 3, 1)

    service(1, lambda: near_y(0), last_own, lambda: near_y(1))
    service(2, lambda: queries_in(0))
    service(3, lambda: sibling_near(0), lambda: sibling_near(1))
    service(4, lambda: far_y(0))
    service(5, lambda: f_recv(0, 6), lambda: queries_in(1), lambda: near_y(2))
    service(6, lambda: partner_done(0), lambda: far_y(1))
    service(7, lambda: f_recv(1, 6), lambda: queries_in(2))
    service(8, lambda: partner_done(1), lambda: sibling_near(2), lambda: far_y(2))
    service(9, lambda: f_recv(2, 6), lambda: combine(0), gathers[0].start)
    service(10, lambda: partner_done(2), gathers[0].cross)
    service(11, lambda: combine(1), gathers[1].start)

    def dispatch(i, keys):
        if len(keys) == 1:
            for step in services[keys[0]]:
                step()
            return
        middle = len(keys) // 2
        pl.when(i < keys[middle])(lambda: dispatch(i, keys[:middle]))
        pl.when(i >= keys[middle])(lambda: dispatch(i, keys[middle:]))

    for i in range(12):
        services.setdefault(i, [])

    def body(i, carry):
        dispatch(i, sorted(services))
        j = i * 2
        at = [step_of(j), step_of(j + 1), step_of(jnp.minimum(j + 2, 23))]
        for n in range(2):
            (h, side, even, odd), (h_, side_, even_, _) = at[n], at[n + 1]
            score(h, side, odd, 1)
            soft(h, side, even, 0)
            score(h_, side_, even_, 0)
            soft(h, side, odd, 1)
        return carry

    lax.fori_loop(0, 12, body, 0)

    def gathered(h):
        arrived(att.at[h, 0], c_rsem.at[h, 6])

    def project_out(h):
        rows = jnp.concatenate(
            [att[h, c_, z0].reshape(512, 128) for c_ in range(2) for z0 in range(4)], axis=1
        )
        weights = jnp.concatenate(
            [wo[((xl + c_) % 2 * 4 + z0) * 3 + h] for c_ in range(2) for z0 in range(4)], axis=0
        )
        total = jnp.dot(rows, weights, preferred_element_type=F32)
        oacc[...] = total if h == 0 else oacc[...] + total

    gathers[0].wave1()
    gathers[0].wave2()
    w_copies[3].wait()
    combine(2)
    gathers[2].start()
    gathers[2].far()
    gathers[1].wave1()
    gathers[0].wave3()
    gathers[1].wave2()
    gathers[1].cross()
    gathers[2].near()
    gathers[1].wave3()
    gathers[2].wave2()
    gathers[2].wave3_x()
    gathers[2].cross()
    gathered(0)
    project_out(0)
    gathered(1)
    project_out(1)
    gathered(2)
    project_out(2)

    outb[...] = oacc[...].astype(BF16).reshape(16, 32, 384)
    for d in (2, 1, 3, 0):
        zd = (z + d) % 4
        send(outb.at[8 + zd], drec.at[0, u], s_sem.at[6], d_rsem.at[0], device(xm, y, zd, core))
        send(outb.at[4 + zd], drec.at[1, u], s_sem.at[6], d_rsem.at[0], device(xp, y, zd, core))
        if d:
            dev = device(x, y, zd, core)
            send(outb.at[zd], drec.at[0, u], s_sem.at[6], d_rsem.at[0], dev)
            send(outb.at[12 + zd], drec.at[1, u], s_sem.at[6], d_rsem.at[0], dev)
    drec[0, u] = outb[z]
    drec[1, u] = outb[12 + z]
    arrived(outb.at[pl.ds(0, 14)], d_rsem.at[0])
    for v in range(8):
        cols = pl.ds(v * 384, 384)
        out_ref[:, cols] = jnp.concatenate([drec[0, v], drec[1, v]], axis=0)

    for n, group in enumerate((
        mod.at[pl.ds(0, 14)], kv.at[:, pl.ds(0, 7)], q.at[0], osend, stsend,
        kv.at[:, pl.ds(0, 7), pl.ds(0, 2)], outb.at[pl.ds(0, 14)],
    )):
        make(group, group, s_sem.at[n], d_rsem.at[0], dev_zp).wait_send()


def local(tokens, mod_shift, mod_scale, mod_gate, qkv_weight, query_gain, key_gain, out_weight):
    vm = pl.BlockSpec(memory_space=pltpu.VMEM)
    anyspace = pl.BlockSpec(memory_space=pl.ANY)
    dma = pltpu.SemaphoreType.DMA
    branch = pl.pallas_call(
        kernel,
        out_shape=pltpu.VMEM(tokens.shape, BF16),
        in_specs=[vm] * 5 + [anyspace] * 2,
        out_specs=vm,
        scratch_shapes=[
            pltpu.VMEM((3072, 1152), BF16),
            pltpu.VMEM((24, 128, 384), BF16),
            pltpu.VMEM((16, 32, 3072), BF16),
            pltpu.VMEM((2, 3, 16, 32, 128), BF16),
            pltpu.VMEM((3, 8, 4, 2, 128, 128), BF16),
            pltpu.VMEM((3, 2, 4, 2, 256, 128), BF16),
            pltpu.VMEM((16, 32, 384), BF16),
            pltpu.VMEM((2, 8, 32, 384), BF16),
            pltpu.VMEM((6, 1, 512), F32),
            pltpu.VMEM((6, 1, 512), F32),
            pltpu.VMEM((6, 128, 512), F32),
            pltpu.VMEM((2, 512, 512), F32),
            pltpu.VMEM((6, 256, 512), BF16),
            pltpu.VMEM((3, 128, 512), BF16),
            pltpu.VMEM((3, 128, 512), BF16),
            pltpu.VMEM((3, 8, 512), F32),
            pltpu.VMEM((3, 8, 512), F32),
            pltpu.VMEM((512, 384), F32),
            dma((4,)),
            dma((7,)),
            dma((24,)),
            dma((8,)),
            dma((3, 4)),
            dma((3,)),
            dma((2, 3)),
            dma((3, 7)),
            dma((1,)),
        ],
        compiler_params=pltpu.CompilerParams(
            collective_id=0, has_side_effects=True, vmem_limit_bytes=60 * 1024 * 1024
        ),
        name="joint_attention",
    )(
        tokens, mod_shift.reshape(1, -1), mod_scale.reshape(1, -1),
        query_gain.reshape(1, -1), key_gain.reshape(1, -1), qkv_weight, out_weight.reshape(24, 128, 384),
    )
    return (tokens.astype(F32) + mod_gate * branch.astype(F32)).astype(BF16)


def solution(mesh):
    in_specs = (
        P(("blk", "ulysses"), None),
        P(),
        P(),
        P(),
        P(None, None, "ulysses"),
        P(),
        P(),
        P(None, "ulysses"),
    )
    out_specs = P(("blk", "ulysses"), None)
    return jax.shard_map(local, mesh=mesh, in_specs=in_specs, out_specs=out_specs, check_vma=False)
```

```python
import math

import jax
import jax.numpy as jnp
from jax import lax
from jax.experimental import pallas as pl
from jax.experimental.pallas import tpu as pltpu
from jax.sharding import PartitionSpec as P

MESH = pl.DeviceIdType.MESH
F32 = jnp.float32
BF16 = jnp.bfloat16
LOG2E = math.log2(math.e)


def kernel(
    tokens_ref, shift_ref, scale_ref, qgain_ref, kgain_ref, w_hbm, wo_hbm,
    out_ref,
    w, wo, mod, q, kv, att, outb, drec, m_s, l_s, acc, s_s, qt, osend, orecv, stsend, strecv, oacc,
    w_sem, s_sem, a_rsem, ob_rsem, f_rsem, q_rsem, e_rsem, c_rsem, d_rsem,
):
    blk = lax.axis_index("blk")
    u = lax.axis_index("ulysses")
    y, xh, core = blk // 4, (blk // 2) % 2, blk % 2
    xl, z = u // 4, u % 4
    x = xh * 2 + xl

    def device(x_, y_, z_, c_):
        return (y_ * 4 + (x_ // 2) * 2 + c_, (x_ % 2) * 4 + z_)

    zp, zm, z2 = (z + 1) % 4, (z + 3) % 4, (z + 2) % 4
    xp, xm, x2 = (x + 1) % 4, (x + 3) % 4, (x + 2) % 4
    yp, ym = (y + 1) % 4, (y + 3) % 4
    dev_zp, dev_zm = device(x, y, zp, core), device(x, y, zm, core)
    dev_xp, dev_xm = device(xp, y, z, core), device(xm, y, z, core)
    dev_x2 = device(x2, y, z, core)
    dev_z2 = device(x, y, z2, core)
    dev_yp, dev_ym = device(x, yp, z, core), device(x, ym, z, core)
    dev_core = device(x, y, z, 1 - core)

    barrier = pltpu.get_barrier_semaphore()
    partners = [dev_yp, dev_ym, dev_x2, dev_core]
    for d in range(4):
        zd = (z + d) % 4
        if d:
            partners.append(device(x, y, zd, core))
        partners.append(device(xp, y, zd, core))
        partners.append(device(xm, y, zd, core))
    for p in partners:
        pl.semaphore_signal(barrier, inc=1, device_id=p, device_id_type=MESH)

    w_copies = [
        pltpu.make_async_copy(w_hbm.at[j], w.at[:, pl.ds(j * 384, 384)], w_sem.at[j]) for j in range(3)
    ]
    w_copies.append(pltpu.make_async_copy(wo_hbm, wo, w_sem.at[3]))
    for c_ in w_copies:
        c_.start()

    wide = tokens_ref[...].astype(F32)
    center = jnp.mean(wide, axis=-1, keepdims=True)
    spread = jnp.mean((wide - center) ** 2, axis=-1, keepdims=True)
    normed = (wide - center) / jnp.sqrt(spread + 1e-06)
    modulated = (normed * (1.0 + scale_ref[...]) + shift_ref[...]).astype(BF16)
    mod[z] = modulated[:32]
    mod[12 + z] = modulated[32:]

    pl.semaphore_wait(barrier, len(partners))

    def make(src, dst, ssem, rsem, dev):
        return pltpu.make_async_remote_copy(
            src_ref=src, dst_ref=dst, send_sem=ssem, recv_sem=rsem, device_id=dev, device_id_type=MESH
        )

    def send(src, dst, ssem, rsem, dev):
        make(src, dst, ssem, rsem, dev).start()

    def arrived(dst, rsem):
        make(dst, dst, s_sem.at[0], rsem, dev_zp).wait_recv()

    class Gather:
        def __init__(self, own_a, own_b, from_minus, from_plus, ssem, rsem, slots=range(24)):
            self.a, self.b, self.fm, self.fp = own_a, own_b, from_minus, from_plus
            self.ssem, self.rsem, self.slots = ssem, rsem, slots

        def send(self, t, src, dst, dev):
            send(src, dst, self.ssem, self.rsem.at[self.slots[t]], dev)

        def recv(self, t, dst):
            arrived(dst, self.rsem.at[self.slots[t]])

        def start_split(self):
            for i in range(2):
                part = pl.ds(i * 16, 16)
                self.send(14 if i else 0, self.a(z).at[part], self.a(z).at[part], dev_zp)
                self.send(15 if i else 2, self.b(z).at[part], self.b(z).at[part], dev_zm)
            self.send(4, self.a(z), self.fm(z), dev_xp)
            self.send(5, self.b(z), self.fp(z), dev_xm)
            for i in range(2):
                part = pl.ds(i * 16, 16)
                self.send(18 if i else 1, self.b(z).at[part], self.b(z).at[part], dev_zp)
                self.send(19 if i else 3, self.a(z).at[part], self.a(z).at[part], dev_zm)

        def wave2_split(self):
            for i in range(2):
                part = pl.ds(i * 16, 16)
                self.recv(19 if i else 3, self.a(zp).at[part])
                self.send(20 if i else 10, self.a(zp).at[part], self.fm(zp).at[part], dev_xp)
                self.recv(18 if i else 1, self.b(zm).at[part])
                self.send(21 if i else 11, self.b(zm).at[part], self.fp(zm).at[part], dev_xm)

        def wave1_split(self):
            for i in range(2):
                part = pl.ds(i * 16, 16)
                self.recv(14 if i else 0, self.a(zm).at[part])
                self.send(16 if i else 7, self.a(zm).at[part], self.fm(zm).at[part], dev_xp)
                self.recv(15 if i else 2, self.b(zp).at[part])
                self.send(17 if i else 9, self.b(zp).at[part], self.fp(zp).at[part], dev_xm)
            self.send(6, self.a(zm), self.a(zm), dev_zp)
            self.send(8, self.b(zp), self.b(zp), dev_zm)

        def x_near_split(self):
            for i in range(2):
                part = pl.ds(i * 16, 16)
                self.recv(16 if i else 7, self.fm(zm).at[part])
                self.recv(17 if i else 9, self.fp(zp).at[part])
                self.recv(20 if i else 10, self.fm(zp).at[part])
                self.recv(21 if i else 11, self.fp(zm).at[part])

        def start(self):
            self.send(0, self.a(z), self.a(z), dev_zp)
            self.send(2, self.b(z), self.b(z), dev_zm)
            self.send(1, self.b(z), self.b(z), dev_zp)
            self.send(3, self.a(z), self.a(z), dev_zm)

        def far(self):
            self.send(6, self.a(z), self.a(z), dev_z2)
            self.send(8, self.b(z), self.b(z), dev_z2)

        def near(self):
            self.recv(0, self.a(zm))
            self.send(7, self.a(zm), self.fm(zm), dev_xp)
            self.recv(2, self.b(zp))
            self.send(9, self.b(zp), self.fp(zp), dev_xm)

        def cross(self):
            self.send(4, self.a(z), self.fm(z), dev_xp)
            self.send(5, self.b(z), self.fp(z), dev_xm)

        def wave3_x(self):
            self.recv(6, self.a(z2))
            self.send(12, self.a(z2), self.fm(z2), dev_xp)
            self.recv(8, self.b(z2))
            self.send(13, self.b(z2), self.fp(z2), dev_xm)

        def wave1(self):
            self.recv(0, self.a(zm))
            self.send(7, self.a(zm), self.fm(zm), dev_xp)
            self.send(6, self.a(zm), self.a(zm), dev_zp)
            self.recv(2, self.b(zp))
            self.send(9, self.b(zp), self.fp(zp), dev_xm)
            self.send(8, self.b(zp), self.b(zp), dev_zm)

        def x_own(self):
            self.recv(4, self.fm(z))
            self.recv(5, self.fp(z))

        def wave2(self):
            self.recv(3, self.a(zp))
            self.send(10, self.a(zp), self.fm(zp), dev_xp)
            self.recv(1, self.b(zm))
            self.send(11, self.b(zm), self.fp(zm), dev_xm)

        def wave3(self):
            self.recv(7, self.fm(zm))
            self.send(12, self.fm(zm), self.fm(zm), dev_zp)
            self.recv(9, self.fp(zp))
            self.send(13, self.fp(zp), self.fp(zp), dev_zm)

        def wave3_split(self):
            part = pl.ds(16, 16)
            self.recv(16, self.fm(zm).at[part])
            self.send(22, self.fm(zm).at[part], self.fm(zm).at[part], dev_zp)
            self.recv(17, self.fp(zp).at[part])
            self.send(23, self.fp(zp).at[part], self.fp(zp).at[part], dev_zm)
            part = pl.ds(0, 16)
            self.recv(6, self.a(z2))
            self.send(12, self.a(z2).at[part], self.fm(z2).at[part], dev_xp)
            self.recv(8, self.b(z2))
            self.send(13, self.b(z2).at[part], self.fp(z2).at[part], dev_xm)

        def x_near_split(self):
            for i in range(2):
                part = pl.ds(i * 16, 16)
                if i == 0:
                    self.recv(7, self.fm(zm).at[part])
                    self.recv(9, self.fp(zp).at[part])
                self.recv(20 if i else 10, self.fm(zp).at[part])
                self.recv(21 if i else 11, self.fp(zm).at[part])

        def x_far_split(self):
            for i in range(2):
                part = pl.ds(i * 16, 16)
                self.recv(22 if i else 12, self.fm(z2).at[part])
                self.recv(23 if i else 13, self.fp(z2).at[part])

    factor = 1.0 / math.sqrt(128)

    def head_norm(value, gain):
        meansq = jnp.mean(value * value, axis=-1, keepdims=True)
        return value * lax.rsqrt(meansq + 1e-06) * gain

    def project(g, pieces):
        rows = jnp.concatenate([mod[p] for p in pieces], axis=0)
        sums = jnp.dot(rows, w[...], preferred_element_type=F32)
        for h in range(3):
            qh = (head_norm(sums[:, h * 128:h * 128 + 128], qgain_ref[...]) * factor).astype(BF16)
            for i, p in enumerate(pieces):
                q[0, h, p] = qh[i * 32:i * 32 + 32]
            kh = head_norm(sums[:, 384 + h * 128:384 + h * 128 + 128], kgain_ref[...])
            kv[h, 0, g, 0] = kh.astype(BF16)
            vh = sums[:, 768 + h * 128:768 + h * 128 + 128]
            kv[h, 0, g, 1] = vh.T.astype(BF16)

    def o_send(h, g, k):
        slot, dev = ((3, dev_yp), (1, dev_ym), (4, dev_core))[k]
        sem = (1 + h if g else 0, 4 + h, 7)[k]
        send(kv.at[h, 0, g], kv.at[h, slot, g], s_sem.at[1], ob_rsem.at[sem], dev)

    def f_send(h, k):
        if k < 4:
            src, dst, dev = kv.at[h, 1 if k % 2 else 3, k], kv.at[h, 2, k], dev_ym if k % 2 else dev_yp
        else:
            slot = (3, 1, 2)[k - 4]
            src, dst, dev = kv.at[h, slot], kv.at[h, slot + 4], dev_core
        send(src, dst, s_sem.at[1], f_rsem.at[h, max(k - 3, 0)], dev)

    def f_recv(h, k):
        arrived(kv.at[h, (7, 5, 6)[k - 4]], f_rsem.at[h, k - 3])

    def own_block(g, heads=(0, 1, 2)):
        for h in heads:
            for k in range(3):
                o_send(h, g, k)

    ga = Gather(
        lambda i: mod.at[i], lambda i: mod.at[12 + i], lambda i: mod.at[8 + i], lambda i: mod.at[4 + i],
        s_sem.at[0], a_rsem,
    )
    ga.start_split()
    ga.wave1_split()
    ga.x_own()
    for c_ in w_copies[:3]:
        c_.wait()
    project(0, [z, 12 + z, 8 + z, 4 + z])
    own_block(0)
    ga.wave2_split()
    project(1, [zm, 12 + zm, zp, 12 + zp])
    own_block(1)
    ga.wave3_split()
    ga.x_near_split()
    project(2, [8 + zm, 4 + zm, 8 + zp, 4 + zp])
    own_block(2)
    ga.x_far_split()
    project(3, [z2, 12 + z2, 8 + z2, 4 + z2])
    for h in range(3):
        o_send(h, 3, 2)
    for h in range(3):
        if h < 2:
            o_send(h, 3, 0)
            o_send(h, 3, 1)
        send(q.at[0, h], q.at[1, h], s_sem.at[2], q_rsem.at[h], dev_x2)

    arrived(kv.at[:, 3, 0], ob_rsem.at[0])
    f_send(0, 0)

    def near_y(h):
        if h:
            f_send(h, 0)
        arrived(kv.at[h, 1], ob_rsem.at[4 + h])
        f_send(h, 1)
        f_send(h, 3)
        f_send(h, 5)
        arrived(kv.at[h, 3, pl.ds(1, 3)], ob_rsem.at[1 + h])
        f_send(h, 2)
        f_send(h, 4)

    def far_y(h):
        arrived(kv.at[h, 2], f_rsem.at[h, 0])
        f_send(h, 6)

    def sibling_near(h):
        f_recv(h, 4)
        f_recv(h, 5)

    def queries_in(h):
        arrived(q.at[1, h], q_rsem.at[h])
        split_queries(h, 1)

    own_keys, near_keys, sibling_keys, far_keys = range(4)
    order = [(0, 0, own_keys), (1, 0, own_keys), (2, 0, own_keys), (0, 0, near_keys)]
    order += [(1, 0, near_keys), (0, 1, own_keys), (0, 1, near_keys), (0, 1, sibling_keys)]
    order += [(0, 0, sibling_keys), (1, 0, sibling_keys), (0, 1, far_keys), (0, 0, far_keys)]
    order += [(1, 1, own_keys), (1, 1, near_keys), (1, 1, sibling_keys), (1, 1, far_keys)]
    order += [(2, 1, own_keys), (2, 1, near_keys), (2, 1, sibling_keys), (2, 1, far_keys)]
    order += [(1, 0, far_keys), (2, 0, near_keys), (2, 0, sibling_keys), (2, 0, far_keys)]
    codes = [(h * 2 + side) * 4 + k for h, side, k in order]
    words = [sum(c << (5 * n) for n, c in enumerate(codes[w * 6:w * 6 + 6])) for w in range(4)]

    def step_of(j):
        w = j // 6
        word = jnp.where(w < 2, jnp.where(w < 1, words[0], words[1]), jnp.where(w < 3, words[2], words[3]))
        code = jnp.right_shift(word, 5 * (j % 6)) % 32
        i, k = code // 4, code % 4
        return i // 2, i % 2, k + 3 * (k // 2) - 4 * (k // 3), 4 - k + 5 * (k // 2)

    def split_queries(h, side):
        wide_q = q[side, h].reshape(512, 128).astype(F32) * LOG2E
        high = wide_q.astype(BF16)
        low = (wide_q - high.astype(F32)).astype(BF16)
        qt[h * 2 + side] = jnp.concatenate([high, low], axis=1).T

    def score(h, side, slot, buf):
        keys = jnp.concatenate([kv[h, slot, g, 0] for g in range(4)], axis=0)
        keys = jnp.concatenate([keys, keys], axis=1)
        s_s[buf] = jnp.dot(keys, qt[h * 2 + side], preferred_element_type=F32)

    def soft(h, side, slot, buf):
        vals = jnp.concatenate([kv[h, slot, g, 1] for g in range(4)], axis=1)
        i = h * 2 + side
        scores = s_s[buf]
        old = m_s[i]
        new = jnp.maximum(old, jnp.max(scores, axis=0, keepdims=True))
        rescale = jnp.exp2(old - new)
        powers = jnp.exp2(scores - new)
        m_s[i] = new
        l_s[i] = l_s[i] * rescale + jnp.sum(powers, axis=0, keepdims=True)
        acc[i] = acc[i] * rescale + jnp.dot(vals, powers.astype(BF16), preferred_element_type=F32)

    def partner_done(h):
        i = h * 2 + 1
        osend[h] = (acc[i] / l_s[i]).astype(BF16)
        stsend[h, 0:1] = m_s[i]
        stsend[h, 1:2] = l_s[i]
        send(osend.at[h], orecv.at[h], s_sem.at[3], e_rsem.at[0, h], dev_x2)
        send(stsend.at[h], strecv.at[h], s_sem.at[4], e_rsem.at[1, h], dev_x2)

    def combine(h):
        i = h * 2
        arrived(orecv.at[h], e_rsem.at[0, h])
        arrived(strecv.at[h], e_rsem.at[1, h])
        other_m, other_l = strecv[h, 0:1], strecv[h, 1:2]
        top = jnp.maximum(m_s[i], other_m)
        mine = jnp.exp2(m_s[i] - top)
        theirs = jnp.exp2(other_m - top) * other_l
        inverse = 1.0 / (l_s[i] * mine + theirs)
        result = acc[i] * (mine * inverse) + orecv[h].astype(F32) * (theirs * inverse)
        result = result.T.astype(BF16)
        att[h, 0, z, 0] = result[:256]
        att[h, 0, z, 1] = result[256:]

    gathers = []
    for h in range(3):
        gc = Gather(
            lambda i, h=h: att.at[h, 0, i, 0], lambda i, h=h: att.at[h, 0, i, 1],
            lambda i, h=h: att.at[h, 1, i, 1], lambda i, h=h: att.at[h, 1, i, 0],
            s_sem.at[5], c_rsem.at[h],
            (0, 1, 2, 3, 6, 6, 4, 6, 5, 6, 6, 6, 6, 6) if h == 2 else (0, 1, 2, 3, 6, 6, 6, 4, 6, 5, 6, 6, 6, 6),
        )
        gathers.append(gc)

    for h in range(3):
        split_queries(h, 0)
    m_s[...] = jnp.full_like(m_s, -1e30)
    l_s[...] = jnp.zeros_like(l_s)
    acc[...] = jnp.zeros_like(acc)
    score(0, 0, 0, 0)
    arrived(kv.at[:, 4], ob_rsem.at[7])

    services = {}

    def service(j, *steps):
        services.setdefault(j, []).extend(steps)

    def last_own():
        o_send(2, 3, 0)
        o_send(2, 3, 1)

    service(1, lambda: near_y(0), last_own, lambda: near_y(1))
    service(2, lambda: queries_in(0))
    service(3, lambda: sibling_near(0), lambda: sibling_near(1))
    service(4, lambda: far_y(0))
    service(5, lambda: f_recv(0, 6), lambda: queries_in(1), lambda: near_y(2))
    service(6, lambda: partner_done(0), lambda: far_y(1))
    service(7, lambda: f_recv(1, 6), lambda: queries_in(2))
    service(8, lambda: partner_done(1), lambda: sibling_near(2), lambda: far_y(2))
    service(9, lambda: f_recv(2, 6), lambda: combine(0), gathers[0].start)
    service(10, lambda: partner_done(2), gathers[0].cross)
    service(11, lambda: combine(1), gathers[1].start)

    def dispatch(i, keys):
        if len(keys) == 1:
            for step in services[keys[0]]:
                step()
            return
        middle = len(keys) // 2
        pl.when(i < keys[middle])(lambda: dispatch(i, keys[:middle]))
        pl.when(i >= keys[middle])(lambda: dispatch(i, keys[middle:]))

    for i in range(12):
        services.setdefault(i, [])

    def body(i, carry):
        dispatch(i, sorted(services))
        j = i * 2
        at = [step_of(j), step_of(j + 1), step_of(jnp.minimum(j + 2, 23))]
        for n in range(2):
            (h, side, even, odd), (h_, side_, even_, _) = at[n], at[n + 1]
            score(h, side, odd, 1)
            soft(h, side, even, 0)
            score(h_, side_, even_, 0)
            soft(h, side, odd, 1)
        return carry

    lax.fori_loop(0, 12, body, 0)

    def gathered(h):
        arrived(att.at[h, 0], c_rsem.at[h, 6])

    def project_out(h):
        rows = jnp.concatenate(
            [att[h, c_, z0].reshape(512, 128) for c_ in range(2) for z0 in range(4)], axis=1
        )
        weights = jnp.concatenate(
            [wo[((xl + c_) % 2 * 4 + z0) * 3 + h] for c_ in range(2) for z0 in range(4)], axis=0
        )
        total = jnp.dot(rows, weights, preferred_element_type=F32)
        oacc[...] = total if h == 0 else oacc[...] + total

    gathers[0].wave1()
    gathers[0].wave2()
    w_copies[3].wait()
    combine(2)
    gathers[2].start()
    gathers[2].far()
    gathers[1].wave1()
    gathers[0].wave3()
    gathers[1].wave2()
    gathers[1].cross()
    gathers[2].near()
    gathers[1].wave3()
    gathers[2].wave2()
    gathers[2].wave3_x()
    gathers[2].cross()
    gathered(0)
    project_out(0)
    gathered(1)
    project_out(1)
    gathered(2)
    project_out(2)

    outb[...] = oacc[...].astype(BF16).reshape(16, 32, 384)
    for d in (2, 1, 3, 0):
        zd = (z + d) % 4
        send(outb.at[8 + zd], drec.at[0, u], s_sem.at[6], d_rsem.at[0], device(xm, y, zd, core))
        send(outb.at[4 + zd], drec.at[1, u], s_sem.at[6], d_rsem.at[0], device(xp, y, zd, core))
        if d:
            dev = device(x, y, zd, core)
            send(outb.at[zd], drec.at[0, u], s_sem.at[6], d_rsem.at[0], dev)
            send(outb.at[12 + zd], drec.at[1, u], s_sem.at[6], d_rsem.at[0], dev)
    drec[0, u] = outb[z]
    drec[1, u] = outb[12 + z]
    arrived(outb.at[pl.ds(0, 14)], d_rsem.at[0])
    for v in range(8):
        cols = pl.ds(v * 384, 384)
        out_ref[:, cols] = jnp.concatenate([drec[0, v], drec[1, v]], axis=0)

    for n, group in enumerate((
        mod.at[pl.ds(0, 14)], kv.at[:, pl.ds(0, 7)], q.at[0], osend, stsend,
        kv.at[:, pl.ds(0, 7), pl.ds(0, 2)], outb.at[pl.ds(0, 14)],
    )):
        make(group, group, s_sem.at[n], d_rsem.at[0], dev_zp).wait_send()


def local(tokens, mod_shift, mod_scale, mod_gate, qkv_weight, query_gain, key_gain, out_weight):
    vm = pl.BlockSpec(memory_space=pltpu.VMEM)
    anyspace = pl.BlockSpec(memory_space=pl.ANY)
    dma = pltpu.SemaphoreType.DMA
    branch = pl.pallas_call(
        kernel,
        out_shape=pltpu.VMEM(tokens.shape, BF16),
        in_specs=[vm] * 5 + [anyspace] * 2,
        out_specs=vm,
        scratch_shapes=[
            pltpu.VMEM((3072, 1152), BF16),
            pltpu.VMEM((24, 128, 384), BF16),
            pltpu.VMEM((16, 32, 3072), BF16),
            pltpu.VMEM((2, 3, 16, 32, 128), BF16),
            pltpu.VMEM((3, 8, 4, 2, 128, 128), BF16),
            pltpu.VMEM((3, 2, 4, 2, 256, 128), BF16),
            pltpu.VMEM((16, 32, 384), BF16),
            pltpu.VMEM((2, 8, 32, 384), BF16),
            pltpu.VMEM((6, 1, 512), F32),
            pltpu.VMEM((6, 1, 512), F32),
            pltpu.VMEM((6, 128, 512), F32),
            pltpu.VMEM((2, 512, 512), F32),
            pltpu.VMEM((6, 256, 512), BF16),
            pltpu.VMEM((3, 128, 512), BF16),
            pltpu.VMEM((3, 128, 512), BF16),
            pltpu.VMEM((3, 8, 512), F32),
            pltpu.VMEM((3, 8, 512), F32),
            pltpu.VMEM((512, 384), F32),
            dma((4,)),
            dma((7,)),
            dma((24,)),
            dma((8,)),
            dma((3, 4)),
            dma((3,)),
            dma((2, 3)),
            dma((3, 7)),
            dma((1,)),
        ],
        compiler_params=pltpu.CompilerParams(
            collective_id=0, has_side_effects=True, vmem_limit_bytes=60 * 1024 * 1024
        ),
        name="joint_attention",
    )(
        tokens, mod_shift.reshape(1, -1), mod_scale.reshape(1, -1),
        query_gain.reshape(1, -1), key_gain.reshape(1, -1), qkv_weight, out_weight.reshape(24, 128, 384),
    )
    return (tokens.astype(F32) + mod_gate * branch.astype(F32)).astype(BF16)


def solution(mesh):
    in_specs = (
        P(("blk", "ulysses"), None),
        P(),
        P(),
        P(),
        P(None, None, "ulysses"),
        P(),
        P(),
        P(None, "ulysses"),
    )
    out_specs = P(("blk", "ulysses"), None)
    return jax.shard_map(local, mesh=mesh, in_specs=in_specs, out_specs=out_specs, check_vma=False)
```

```python
import math

import jax
import jax.numpy as jnp
from jax import lax
from jax.experimental import pallas as pl
from jax.experimental.pallas import tpu as pltpu
from jax.sharding import PartitionSpec as P

MESH = pl.DeviceIdType.MESH
F32 = jnp.float32
BF16 = jnp.bfloat16
LOG2E = math.log2(math.e)


def kernel(
    tokens_ref, shift_ref, scale_ref, qgain_ref, kgain_ref, w_hbm, wo_hbm,
    out_ref,
    w, wo, mod, q, kv, att, outb, drec, m_s, l_s, acc, s_s, qt, osend, orecv, stsend, strecv, oacc,
    w_sem, s_sem, a_rsem, ob_rsem, f_rsem, q_rsem, e_rsem, c_rsem, d_rsem,
):
    blk = lax.axis_index("blk")
    u = lax.axis_index("ulysses")
    y, xh, core = blk // 4, (blk // 2) % 2, blk % 2
    xl, z = u // 4, u % 4
    x = xh * 2 + xl

    def device(x_, y_, z_, c_):
        return (y_ * 4 + (x_ // 2) * 2 + c_, (x_ % 2) * 4 + z_)

    zp, zm, z2 = (z + 1) % 4, (z + 3) % 4, (z + 2) % 4
    xp, xm, x2 = (x + 1) % 4, (x + 3) % 4, (x + 2) % 4
    yp, ym = (y + 1) % 4, (y + 3) % 4
    dev_zp, dev_zm = device(x, y, zp, core), device(x, y, zm, core)
    dev_xp, dev_xm = device(xp, y, z, core), device(xm, y, z, core)
    dev_x2 = device(x2, y, z, core)
    dev_z2 = device(x, y, z2, core)
    dev_yp, dev_ym = device(x, yp, z, core), device(x, ym, z, core)
    dev_core = device(x, y, z, 1 - core)

    barrier = pltpu.get_barrier_semaphore()
    partners = [dev_yp, dev_ym, dev_x2, dev_core]
    for d in range(4):
        zd = (z + d) % 4
        if d:
            partners.append(device(x, y, zd, core))
        partners.append(device(xp, y, zd, core))
        partners.append(device(xm, y, zd, core))
    for p in partners:
        pl.semaphore_signal(barrier, inc=1, device_id=p, device_id_type=MESH)

    w_copies = [
        pltpu.make_async_copy(w_hbm.at[j], w.at[:, pl.ds(j * 384, 384)], w_sem.at[j]) for j in range(3)
    ]
    w_copies.append(pltpu.make_async_copy(wo_hbm, wo, w_sem.at[3]))
    for c_ in w_copies:
        c_.start()

    wide = tokens_ref[...].astype(F32)
    center = jnp.mean(wide, axis=-1, keepdims=True)
    spread = jnp.mean((wide - center) ** 2, axis=-1, keepdims=True)
    normed = (wide - center) / jnp.sqrt(spread + 1e-06)
    modulated = (normed * (1.0 + scale_ref[...]) + shift_ref[...]).astype(BF16)
    mod[z] = modulated[:32]
    mod[12 + z] = modulated[32:]

    pl.semaphore_wait(barrier, len(partners))

    def make(src, dst, ssem, rsem, dev):
        return pltpu.make_async_remote_copy(
            src_ref=src, dst_ref=dst, send_sem=ssem, recv_sem=rsem, device_id=dev, device_id_type=MESH
        )

    def send(src, dst, ssem, rsem, dev):
        make(src, dst, ssem, rsem, dev).start()

    def arrived(dst, rsem):
        make(dst, dst, s_sem.at[0], rsem, dev_zp).wait_recv()

    class Gather:
        def __init__(self, own_a, own_b, from_minus, from_plus, ssem, rsem, slots=range(24)):
            self.a, self.b, self.fm, self.fp = own_a, own_b, from_minus, from_plus
            self.ssem, self.rsem, self.slots = ssem, rsem, slots

        def send(self, t, src, dst, dev):
            send(src, dst, self.ssem, self.rsem.at[self.slots[t]], dev)

        def recv(self, t, dst):
            arrived(dst, self.rsem.at[self.slots[t]])

        def start_split(self):
            for i in range(2):
                part = pl.ds(i * 16, 16)
                self.send(14 if i else 0, self.a(z).at[part], self.a(z).at[part], dev_zp)
                self.send(15 if i else 2, self.b(z).at[part], self.b(z).at[part], dev_zm)
            self.send(4, self.a(z), self.fm(z), dev_xp)
            self.send(5, self.b(z), self.fp(z), dev_xm)
            for i in range(2):
                part = pl.ds(i * 16, 16)
                self.send(18 if i else 1, self.b(z).at[part], self.b(z).at[part], dev_zp)
                self.send(19 if i else 3, self.a(z).at[part], self.a(z).at[part], dev_zm)

        def wave2_split(self):
            for i in range(2):
                part = pl.ds(i * 16, 16)
                self.recv(19 if i else 3, self.a(zp).at[part])
                self.send(20 if i else 10, self.a(zp).at[part], self.fm(zp).at[part], dev_xp)
                self.recv(18 if i else 1, self.b(zm).at[part])
                self.send(21 if i else 11, self.b(zm).at[part], self.fp(zm).at[part], dev_xm)

        def wave1_split(self):
            for i in range(2):
                part = pl.ds(i * 16, 16)
                self.recv(14 if i else 0, self.a(zm).at[part])
                self.send(16 if i else 7, self.a(zm).at[part], self.fm(zm).at[part], dev_xp)
                self.recv(15 if i else 2, self.b(zp).at[part])
                self.send(17 if i else 9, self.b(zp).at[part], self.fp(zp).at[part], dev_xm)
            self.send(6, self.a(zm), self.a(zm), dev_zp)
            self.send(8, self.b(zp), self.b(zp), dev_zm)

        def x_near_split(self):
            for i in range(2):
                part = pl.ds(i * 16, 16)
                self.recv(16 if i else 7, self.fm(zm).at[part])
                self.recv(17 if i else 9, self.fp(zp).at[part])
                self.recv(20 if i else 10, self.fm(zp).at[part])
                self.recv(21 if i else 11, self.fp(zm).at[part])

        def start(self):
            self.send(0, self.a(z), self.a(z), dev_zp)
            self.send(2, self.b(z), self.b(z), dev_zm)
            self.send(1, self.b(z), self.b(z), dev_zp)
            self.send(3, self.a(z), self.a(z), dev_zm)

        def far(self):
            self.send(6, self.a(z), self.a(z), dev_z2)
            self.send(8, self.b(z), self.b(z), dev_z2)

        def near(self):
            self.recv(0, self.a(zm))
            self.send(7, self.a(zm), self.fm(zm), dev_xp)
            self.recv(2, self.b(zp))
            self.send(9, self.b(zp), self.fp(zp), dev_xm)

        def cross(self):
            self.send(4, self.a(z), self.fm(z), dev_xp)
            self.send(5, self.b(z), self.fp(z), dev_xm)

        def wave3_x(self):
            self.recv(6, self.a(z2))
            self.send(12, self.a(z2), self.fm(z2), dev_xp)
            self.recv(8, self.b(z2))
            self.send(13, self.b(z2), self.fp(z2), dev_xm)

        def wave1(self):
            self.recv(0, self.a(zm))
            self.send(7, self.a(zm), self.fm(zm), dev_xp)
            self.send(6, self.a(zm), self.a(zm), dev_zp)
            self.recv(2, self.b(zp))
            self.send(9, self.b(zp), self.fp(zp), dev_xm)
            self.send(8, self.b(zp), self.b(zp), dev_zm)

        def x_own(self):
            self.recv(4, self.fm(z))
            self.recv(5, self.fp(z))

        def wave2(self):
            self.recv(3, self.a(zp))
            self.send(10, self.a(zp), self.fm(zp), dev_xp)
            self.recv(1, self.b(zm))
            self.send(11, self.b(zm), self.fp(zm), dev_xm)

        def wave3(self):
            self.recv(7, self.fm(zm))
            self.send(12, self.fm(zm), self.fm(zm), dev_zp)
            self.recv(9, self.fp(zp))
            self.send(13, self.fp(zp), self.fp(zp), dev_zm)

        def wave3_split(self):
            part = pl.ds(16, 16)
            self.recv(16, self.fm(zm).at[part])
            self.send(22, self.fm(zm).at[part], self.fm(zm).at[part], dev_zp)
            self.recv(17, self.fp(zp).at[part])
            self.send(23, self.fp(zp).at[part], self.fp(zp).at[part], dev_zm)
            part = pl.ds(0, 16)
            self.recv(6, self.a(z2))
            self.send(12, self.a(z2).at[part], self.fm(z2).at[part], dev_xp)
            self.recv(8, self.b(z2))
            self.send(13, self.b(z2).at[part], self.fp(z2).at[part], dev_xm)

        def x_near_split(self):
            for i in range(2):
                part = pl.ds(i * 16, 16)
                if i == 0:
                    self.recv(7, self.fm(zm).at[part])
                    self.recv(9, self.fp(zp).at[part])
                self.recv(20 if i else 10, self.fm(zp).at[part])
                self.recv(21 if i else 11, self.fp(zm).at[part])

        def x_far_split(self):
            for i in range(2):
                part = pl.ds(i * 16, 16)
                self.recv(22 if i else 12, self.fm(z2).at[part])
                self.recv(23 if i else 13, self.fp(z2).at[part])

    factor = 1.0 / math.sqrt(128)

    def head_norm(value, gain):
        meansq = jnp.mean(value * value, axis=-1, keepdims=True)
        return value * lax.rsqrt(meansq + 1e-06) * gain

    def project(g, pieces, send_keys):
        rows = jnp.concatenate([mod[p] for p in pieces], axis=0)
        sums = jnp.dot(rows, w[:, 384:], preferred_element_type=F32)
        for h in range(3):
            kh = head_norm(sums[:, h * 128:h * 128 + 128], kgain_ref[...])
            kv[h, 0, g, 0] = kh.astype(BF16)
            vh = sums[:, 384 + h * 128:384 + h * 128 + 128]
            kv[h, 0, g, 1] = vh.T.astype(BF16)
        send_keys()
        sums = jnp.dot(rows, w[:, :384], preferred_element_type=F32)
        for h in range(3):
            qh = (head_norm(sums[:, h * 128:h * 128 + 128], qgain_ref[...]) * factor).astype(BF16)
            for i, p in enumerate(pieces):
                q[0, h, p] = qh[i * 32:i * 32 + 32]

    def o_send(h, g, k):
        slot, dev = ((3, dev_yp), (1, dev_ym), (4, dev_core))[k]
        sem = (1 + h if g else 0, 4 + h, 7)[k]
        send(kv.at[h, 0, g], kv.at[h, slot, g], s_sem.at[1], ob_rsem.at[sem], dev)

    def f_send(h, k):
        if k < 4:
            src, dst, dev = kv.at[h, 1 if k % 2 else 3, k], kv.at[h, 2, k], dev_ym if k % 2 else dev_yp
        else:
            slot = (3, 1, 2)[k - 4]
            src, dst, dev = kv.at[h, slot], kv.at[h, slot + 4], dev_core
        send(src, dst, s_sem.at[1], f_rsem.at[h, max(k - 3, 0)], dev)

    def f_recv(h, k):
        arrived(kv.at[h, (7, 5, 6)[k - 4]], f_rsem.at[h, k - 3])

    def own_block(g, heads=(0, 1, 2)):
        for h in heads:
            for k in range(3):
                o_send(h, g, k)

    ga = Gather(
        lambda i: mod.at[i], lambda i: mod.at[12 + i], lambda i: mod.at[8 + i], lambda i: mod.at[4 + i],
        s_sem.at[0], a_rsem,
    )
    ga.start_split()
    ga.wave1_split()
    ga.x_own()
    for c_ in w_copies[:3]:
        c_.wait()
    project(0, [z, 12 + z, 8 + z, 4 + z], lambda: own_block(0))
    ga.wave2_split()
    project(1, [zm, 12 + zm, zp, 12 + zp], lambda: own_block(1))
    ga.wave3_split()
    ga.x_near_split()
    project(2, [8 + zm, 4 + zm, 8 + zp, 4 + zp], lambda: own_block(2))
    ga.x_far_split()

    def last_block():
        for h in range(3):
            o_send(h, 3, 2)
        for h in range(2):
            o_send(h, 3, 0)
            o_send(h, 3, 1)

    project(3, [z2, 12 + z2, 8 + z2, 4 + z2], last_block)
    for h in range(3):
        send(q.at[0, h], q.at[1, h], s_sem.at[2], q_rsem.at[h], dev_x2)

    arrived(kv.at[:, 3, 0], ob_rsem.at[0])
    f_send(0, 0)

    def near_y(h):
        if h:
            f_send(h, 0)
        arrived(kv.at[h, 1], ob_rsem.at[4 + h])
        f_send(h, 1)
        f_send(h, 3)
        f_send(h, 5)
        arrived(kv.at[h, 3, pl.ds(1, 3)], ob_rsem.at[1 + h])
        f_send(h, 2)
        f_send(h, 4)

    def far_y(h):
        arrived(kv.at[h, 2], f_rsem.at[h, 0])
        f_send(h, 6)

    def sibling_near(h):
        f_recv(h, 4)
        f_recv(h, 5)

    def queries_in(h):
        arrived(q.at[1, h], q_rsem.at[h])
        split_queries(h, 1)

    own_keys, near_keys, sibling_keys, far_keys = range(4)
    order = [(0, 0, own_keys), (1, 0, own_keys), (2, 0, own_keys), (0, 0, near_keys)]
    order += [(1, 0, near_keys), (0, 1, own_keys), (0, 1, near_keys), (0, 1, sibling_keys)]
    order += [(0, 0, sibling_keys), (1, 0, sibling_keys), (0, 1, far_keys), (0, 0, far_keys)]
    order += [(1, 1, own_keys), (1, 1, near_keys), (1, 1, sibling_keys), (1, 1, far_keys)]
    order += [(2, 1, own_keys), (2, 1, near_keys), (2, 1, sibling_keys), (2, 1, far_keys)]
    order += [(1, 0, far_keys), (2, 0, near_keys), (2, 0, sibling_keys), (2, 0, far_keys)]
    codes = [(h * 2 + side) * 4 + k for h, side, k in order]
    words = [sum(c << (5 * n) for n, c in enumerate(codes[w * 6:w * 6 + 6])) for w in range(4)]

    def step_of(j):
        w = j // 6
        word = jnp.where(w < 2, jnp.where(w < 1, words[0], words[1]), jnp.where(w < 3, words[2], words[3]))
        code = jnp.right_shift(word, 5 * (j % 6)) % 32
        i, k = code // 4, code % 4
        return i // 2, i % 2, k + 3 * (k // 2) - 4 * (k // 3), 4 - k + 5 * (k // 2)

    def split_queries(h, side):
        wide_q = q[side, h].reshape(512, 128).astype(F32) * LOG2E
        high = wide_q.astype(BF16)
        low = (wide_q - high.astype(F32)).astype(BF16)
        qt[h * 2 + side] = jnp.concatenate([high, low], axis=1).T

    def score(h, side, slot, buf):
        keys = jnp.concatenate([kv[h, slot, g, 0] for g in range(4)], axis=0)
        keys = jnp.concatenate([keys, keys], axis=1)
        s_s[buf] = jnp.dot(keys, qt[h * 2 + side], preferred_element_type=F32)

    def soft(h, side, slot, buf):
        vals = jnp.concatenate([kv[h, slot, g, 1] for g in range(4)], axis=1)
        i = h * 2 + side
        scores = s_s[buf]
        old = m_s[i]
        new = jnp.maximum(old, jnp.max(scores, axis=0, keepdims=True))
        rescale = jnp.exp2(old - new)
        powers = jnp.exp2(scores - new)
        m_s[i] = new
        l_s[i] = l_s[i] * rescale + jnp.sum(powers, axis=0, keepdims=True)
        acc[i] = acc[i] * rescale + jnp.dot(vals, powers.astype(BF16), preferred_element_type=F32)

    def partner_done(h):
        i = h * 2 + 1
        osend[h] = (acc[i] / l_s[i]).astype(BF16)
        stsend[h, 0:1] = m_s[i]
        stsend[h, 1:2] = l_s[i]
        send(osend.at[h], orecv.at[h], s_sem.at[3], e_rsem.at[0, h], dev_x2)
        send(stsend.at[h], strecv.at[h], s_sem.at[4], e_rsem.at[1, h], dev_x2)

    def combine(h):
        i = h * 2
        arrived(orecv.at[h], e_rsem.at[0, h])
        arrived(strecv.at[h], e_rsem.at[1, h])
        other_m, other_l = strecv[h, 0:1], strecv[h, 1:2]
        top = jnp.maximum(m_s[i], other_m)
        mine = jnp.exp2(m_s[i] - top)
        theirs = jnp.exp2(other_m - top) * other_l
        inverse = 1.0 / (l_s[i] * mine + theirs)
        result = acc[i] * (mine * inverse) + orecv[h].astype(F32) * (theirs * inverse)
        result = result.T.astype(BF16)
        att[h, 0, z, 0] = result[:256]
        att[h, 0, z, 1] = result[256:]

    gathers = []
    for h in range(3):
        gc = Gather(
            lambda i, h=h: att.at[h, 0, i, 0], lambda i, h=h: att.at[h, 0, i, 1],
            lambda i, h=h: att.at[h, 1, i, 1], lambda i, h=h: att.at[h, 1, i, 0],
            s_sem.at[5], c_rsem.at[h],
            (0, 1, 2, 3, 6, 6, 4, 6, 5, 6, 6, 6, 6, 6) if h == 2 else (0, 1, 2, 3, 6, 6, 6, 4, 6, 5, 6, 6, 6, 6),
        )
        gathers.append(gc)

    for h in range(3):
        split_queries(h, 0)
    m_s[...] = jnp.full_like(m_s, -1e30)
    l_s[...] = jnp.zeros_like(l_s)
    acc[...] = jnp.zeros_like(acc)
    score(0, 0, 0, 0)
    arrived(kv.at[:, 4], ob_rsem.at[7])

    services = {}

    def service(j, *steps):
        services.setdefault(j, []).extend(steps)

    def last_own():
        o_send(2, 3, 0)
        o_send(2, 3, 1)

    service(1, lambda: near_y(0), last_own, lambda: near_y(1))
    service(2, lambda: queries_in(0))
    service(3, lambda: sibling_near(0), lambda: sibling_near(1))
    service(4, lambda: far_y(0))
    service(5, lambda: f_recv(0, 6), lambda: queries_in(1), lambda: near_y(2))
    service(6, lambda: partner_done(0), lambda: far_y(1))
    service(7, lambda: f_recv(1, 6), lambda: queries_in(2))
    service(8, lambda: partner_done(1), lambda: sibling_near(2), lambda: far_y(2))
    service(9, lambda: f_recv(2, 6), lambda: combine(0), gathers[0].start)
    service(10, lambda: partner_done(2), gathers[0].cross)
    service(11, lambda: combine(1), gathers[1].start)

    def dispatch(i, keys):
        if len(keys) == 1:
            for step in services[keys[0]]:
                step()
            return
        middle = len(keys) // 2
        pl.when(i < keys[middle])(lambda: dispatch(i, keys[:middle]))
        pl.when(i >= keys[middle])(lambda: dispatch(i, keys[middle:]))

    for i in range(12):
        services.setdefault(i, [])

    def body(i, carry):
        dispatch(i, sorted(services))
        j = i * 2
        at = [step_of(j), step_of(j + 1), step_of(jnp.minimum(j + 2, 23))]
        for n in range(2):
            (h, side, even, odd), (h_, side_, even_, _) = at[n], at[n + 1]
            score(h, side, odd, 1)
            soft(h, side, even, 0)
            score(h_, side_, even_, 0)
            soft(h, side, odd, 1)
        return carry

    lax.fori_loop(0, 12, body, 0)

    def gathered(h):
        arrived(att.at[h, 0], c_rsem.at[h, 6])

    def project_out(h):
        rows = jnp.concatenate(
            [att[h, c_, z0].reshape(512, 128) for c_ in range(2) for z0 in range(4)], axis=1
        )
        weights = jnp.concatenate(
            [wo[((xl + c_) % 2 * 4 + z0) * 3 + h] for c_ in range(2) for z0 in range(4)], axis=0
        )
        total = jnp.dot(rows, weights, preferred_element_type=F32)
        oacc[...] = total if h == 0 else oacc[...] + total

    gathers[0].wave1()
    gathers[0].wave2()
    w_copies[3].wait()
    combine(2)
    gathers[2].start()
    gathers[2].far()
    gathers[1].wave1()
    gathers[0].wave3()
    gathers[1].wave2()
    gathers[1].cross()
    gathers[2].near()
    gathers[1].wave3()
    gathers[2].wave2()
    gathers[2].wave3_x()
    gathers[2].cross()
    gathered(0)
    project_out(0)
    gathered(1)
    project_out(1)
    gathered(2)
    project_out(2)

    outb[...] = oacc[...].astype(BF16).reshape(16, 32, 384)
    for d in (2, 1, 3, 0):
        zd = (z + d) % 4
        send(outb.at[8 + zd], drec.at[0, u], s_sem.at[6], d_rsem.at[0], device(xm, y, zd, core))
        send(outb.at[4 + zd], drec.at[1, u], s_sem.at[6], d_rsem.at[0], device(xp, y, zd, core))
        if d:
            dev = device(x, y, zd, core)
            send(outb.at[zd], drec.at[0, u], s_sem.at[6], d_rsem.at[0], dev)
            send(outb.at[12 + zd], drec.at[1, u], s_sem.at[6], d_rsem.at[0], dev)
    drec[0, u] = outb[z]
    drec[1, u] = outb[12 + z]
    arrived(outb.at[pl.ds(0, 14)], d_rsem.at[0])
    for v in range(8):
        cols = pl.ds(v * 384, 384)
        out_ref[:, cols] = jnp.concatenate([drec[0, v], drec[1, v]], axis=0)

    for n, group in enumerate((
        mod.at[pl.ds(0, 14)], kv.at[:, pl.ds(0, 7)], q.at[0], osend, stsend,
        kv.at[:, pl.ds(0, 7), pl.ds(0, 2)], outb.at[pl.ds(0, 14)],
    )):
        make(group, group, s_sem.at[n], d_rsem.at[0], dev_zp).wait_send()


def local(tokens, mod_shift, mod_scale, mod_gate, qkv_weight, query_gain, key_gain, out_weight):
    vm = pl.BlockSpec(memory_space=pltpu.VMEM)
    anyspace = pl.BlockSpec(memory_space=pl.ANY)
    dma = pltpu.SemaphoreType.DMA
    branch = pl.pallas_call(
        kernel,
        out_shape=pltpu.VMEM(tokens.shape, BF16),
        in_specs=[vm] * 5 + [anyspace] * 2,
        out_specs=vm,
        scratch_shapes=[
            pltpu.VMEM((3072, 1152), BF16),
            pltpu.VMEM((24, 128, 384), BF16),
            pltpu.VMEM((16, 32, 3072), BF16),
            pltpu.VMEM((2, 3, 16, 32, 128), BF16),
            pltpu.VMEM((3, 8, 4, 2, 128, 128), BF16),
            pltpu.VMEM((3, 2, 4, 2, 256, 128), BF16),
            pltpu.VMEM((16, 32, 384), BF16),
            pltpu.VMEM((2, 8, 32, 384), BF16),
            pltpu.VMEM((6, 1, 512), F32),
            pltpu.VMEM((6, 1, 512), F32),
            pltpu.VMEM((6, 128, 512), F32),
            pltpu.VMEM((2, 512, 512), F32),
            pltpu.VMEM((6, 256, 512), BF16),
            pltpu.VMEM((3, 128, 512), BF16),
            pltpu.VMEM((3, 128, 512), BF16),
            pltpu.VMEM((3, 8, 512), F32),
            pltpu.VMEM((3, 8, 512), F32),
            pltpu.VMEM((512, 384), F32),
            dma((4,)),
            dma((7,)),
            dma((24,)),
            dma((8,)),
            dma((3, 4)),
            dma((3,)),
            dma((2, 3)),
            dma((3, 7)),
            dma((1,)),
        ],
        compiler_params=pltpu.CompilerParams(
            collective_id=0, has_side_effects=True, vmem_limit_bytes=60 * 1024 * 1024
        ),
        name="joint_attention",
    )(
        tokens, mod_shift.reshape(1, -1), mod_scale.reshape(1, -1),
        query_gain.reshape(1, -1), key_gain.reshape(1, -1), qkv_weight, out_weight.reshape(24, 128, 384),
    )
    return (tokens.astype(F32) + mod_gate * branch.astype(F32)).astype(BF16)


def solution(mesh):
    in_specs = (
        P(("blk", "ulysses"), None),
        P(),
        P(),
        P(),
        P(None, None, "ulysses"),
        P(),
        P(),
        P(None, "ulysses"),
    )
    out_specs = P(("blk", "ulysses"), None)
    return jax.shard_map(local, mesh=mesh, in_specs=in_specs, out_specs=out_specs, check_vma=False)
```
